16 devices in a mesh: model: 4 (over z, y), data: 4 (over x, core).
Axes of the slice: x: 2, y: 2, z: 2, core: 2. Of those that a mesh axis runs over, the one named last changes fastest.
Arguments:
- grad_qkv: float32 [4, 32, 256, 768], P('data', None, None, 'model')
- weight_qkv: float32 [32, 256, 768], P(None, 'data', 'model')
- moment1_qkv: float32 [32, 256, 768], P(None, 'data', 'model')
- moment2_qkv: float32 [32, 256, 768], P(None, 'data', 'model')
- grad_proj: float32 [4, 32, 256, 256], P('data', None, 'model')
- weight_proj: float32 [32, 256, 256], P(None, ('model', 'data'))
- moment1_proj: float32 [32, 256, 256], P(None, ('model', 'data'))
- moment2_proj: float32 [32, 256, 256], P(None, ('model', 'data'))
- grad_fcin: float32 [4, 32, 256, 1024], P('data', None, None, 'model')
- weight_fcin: float32 [32, 256, 1024], P(None, 'data', 'model')
- moment1_fcin: float32 [32, 256, 1024], P(None, 'data', 'model')
- moment2_fcin: float32 [32, 256, 1024], P(None, 'data', 'model')
- grad_fcout: float32 [4, 32, 1024, 256], P('data', None, 'model')
- weight_fcout: float32 [32, 1024, 256], P(None, ('model', 'data'))
- moment1_fcout: float32 [32, 1024, 256], P(None, ('model', 'data'))
- moment2_fcout: float32 [32, 1024, 256], P(None, ('model', 'data'))
Outputs:
- output 1: bfloat16 [32, 256, 768], P(None, None, 'model')
- output 2: bfloat16 [32, 256, 256], P(None, 'model')
- output 3: bfloat16 [32, 256, 1024], P(None, None, 'model')
- output 4: bfloat16 [32, 1024, 256], P(None, 'model')
- output 5: float32 [32, 256, 768], P(None, 'data', 'model')
- output 6: float32 [32, 256, 256], P(None, ('model', 'data'))
- output 7: float32 [32, 256, 1024], P(None, 'data', 'model')
- output 8: float32 [32, 1024, 256], P(None, ('model', 'data'))
- output 9: float32 [32, 256, 768], P(None, 'data', 'model')
- output 10: float32 [32, 256, 256], P(None, ('model', 'data'))
- output 11: float32 [32, 256, 1024], P(None, 'data', 'model')
- output 12: float32 [32, 1024, 256], P(None, ('model', 'data'))
- output 13: float32 [32, 256, 768], P(None, 'data', 'model')
- output 14: float32 [32, 256, 256], P(None, ('model', 'data'))
- output 15: float32 [32, 256, 1024], P(None, 'data', 'model')
- output 16: float32 [32, 1024, 256], P(None, ('model', 'data'))
All inputs are finite; a program needn't handle non-finite values.
Results may differ from the reference program's by a relative error of at most 0.001.
Values are sent between devices in bfloat16 or wider.
A program may use at most 1 GiB of HBM per device.

```python
import jax
import jax.numpy as jnp

D_MODEL = 256
FF_DIM = 1024
LAYERS = 32
DATA_SIZE = 4
STEP_COUNT = 100

LEARN_RATE = 0.08
BETA_ONE = 0.9
BETA_TWO = 0.999
ADAM_EPS = 1e-6
DECAY_RATE = 0.01
MAX_NORM = 1.0
TILT_RATE = 0.8
KIND_NAMES = ("qkv", "proj", "fcin", "fcout")
KIND_SHAPES = ((D_MODEL, 3 * D_MODEL), (D_MODEL, D_MODEL), (D_MODEL, FF_DIM), (FF_DIM, D_MODEL))


def tilt_profile(num_rows, num_cols):
    row_pos = (jnp.arange(num_rows, dtype=jnp.float32) + 0.5) / num_rows
    col_pos = (jnp.arange(num_cols, dtype=jnp.float32) + 0.5) / num_cols
    row_scale = jnp.exp(TILT_RATE * (2.0 * row_pos - 1.0))
    col_scale = jnp.exp(TILT_RATE * (2.0 * col_pos - 1.0))
    return row_scale[:, None] * col_scale[None, :]


def setup_inputs(seed: int = 0) -> dict:
    base_key = jax.random.key(seed)
    norm_ratio = jax.random.uniform(jax.random.fold_in(base_key, 100), (), jnp.float32, 2.5, 4.5)
    raw_grads = []
    grad_scales = []
    total_sq = jnp.zeros((), jnp.float32)
    for kind_idx, shape_pair in enumerate(KIND_SHAPES):
        num_rows, num_cols = shape_pair
        kind_keys = jax.random.split(jax.random.fold_in(base_key, kind_idx), 7)
        grad_scale = jnp.exp(jax.random.uniform(kind_keys[0], (LAYERS, 1, 1), jnp.float32, -1.1, 1.1))
        common = jax.random.normal(kind_keys[1], (1, LAYERS, num_rows, num_cols), jnp.float32)
        dev_noise = jax.random.normal(kind_keys[2], (DATA_SIZE, LAYERS, num_rows, num_cols), jnp.float32)
        raw_grad = grad_scale * (common + dev_noise)
        mean_grad = jnp.mean(raw_grad, axis=0)
        total_sq = total_sq + jnp.sum(mean_grad * mean_grad)
        raw_grads.append(raw_grad)
        grad_scales.append(grad_scale)
    factor = norm_ratio * MAX_NORM / jnp.sqrt(total_sq)
    inputs = {}
    for kind_idx, shape_pair in enumerate(KIND_SHAPES):
        num_rows, num_cols = shape_pair
        kind_name = KIND_NAMES[kind_idx]
        kind_keys = jax.random.split(jax.random.fold_in(base_key, kind_idx), 7)
        profile = tilt_profile(num_rows, num_cols)
        weight_scale = jnp.exp(jax.random.uniform(kind_keys[3], (LAYERS, 1, 1), jnp.float32, -1.1, 1.1)) * num_rows ** -0.5
        clip_scale = grad_scales[kind_idx] * factor / norm_ratio
        shape_full = (LAYERS, num_rows, num_cols)
        inputs["grad_" + kind_name] = raw_grads[kind_idx] * factor
        inputs["weight_" + kind_name] = jax.random.normal(kind_keys[4], shape_full, jnp.float32) * weight_scale * profile
        inputs["moment1_" + kind_name] = jax.random.normal(kind_keys[5], shape_full, jnp.float32) * clip_scale
        inputs["moment2_" + kind_name] = (clip_scale * profile) ** 2 * jax.random.uniform(kind_keys[6], shape_full, jnp.float32, 0.5, 1.5)
    return inputs


def lamb_tensor(grad_mean, weight, moment1, moment2, clip_coef):
    clipped = clip_coef * grad_mean
    new_first = BETA_ONE * moment1 + (1.0 - BETA_ONE) * clipped
    new_second = BETA_TWO * moment2 + (1.0 - BETA_TWO) * clipped * clipped
    first_hat = new_first / (1.0 - BETA_ONE ** STEP_COUNT)
    second_hat = new_second / (1.0 - BETA_TWO ** STEP_COUNT)
    update = first_hat / (jnp.sqrt(second_hat) + ADAM_EPS) + DECAY_RATE * weight
    weight_norm = jnp.sqrt(jnp.sum(weight * weight, axis=(1, 2), keepdims=True))
    update_norm = jnp.sqrt(jnp.sum(update * update, axis=(1, 2), keepdims=True))
    new_weight = weight - LEARN_RATE * (weight_norm / update_norm) * update
    return new_weight, new_first, new_second


def reference(grad_qkv, weight_qkv, moment1_qkv, moment2_qkv, grad_proj, weight_proj, moment1_proj, moment2_proj, grad_fcin, weight_fcin, moment1_fcin, moment2_fcin, grad_fcout, weight_fcout, moment1_fcout, moment2_fcout):
    grad_list = (grad_qkv, grad_proj, grad_fcin, grad_fcout)
    states = ((weight_qkv, moment1_qkv, moment2_qkv), (weight_proj, moment1_proj, moment2_proj), (weight_fcin, moment1_fcin, moment2_fcin), (weight_fcout, moment1_fcout, moment2_fcout))
    grad_means = [jnp.sum(grad_stack.astype(jnp.bfloat16).astype(jnp.float32), axis=0) / DATA_SIZE for grad_stack in grad_list]
    total_sq = sum(jnp.sum(grad_mean * grad_mean) for grad_mean in grad_means)
    clip_coef = jnp.minimum(1.0, MAX_NORM / jnp.sqrt(total_sq))
    results = [lamb_tensor(grad_means[kind_idx], states[kind_idx][0], states[kind_idx][1], states[kind_idx][2], clip_coef) for kind_idx in range(4)]
    replicas = [outcome[0].astype(jnp.bfloat16) for outcome in results]
    return (replicas[0], replicas[1], replicas[2], replicas[3], results[0][0], results[1][0], results[2][0], results[3][0], results[0][1], results[1][1], results[2][1], results[3][1], results[0][2], results[1][2], results[2][2], results[3][2])
```

```python
import functools

import jax
import jax.numpy as jnp
from jax import lax
from jax.experimental import pallas as pl
from jax.experimental.pallas import tpu as pltpu
from jax.sharding import PartitionSpec as P

LEARN_RATE = 0.08
BETA_ONE = 0.9
BETA_TWO = 0.999
ADAM_EPS = 1e-6
DECAY_RATE = 0.01
MAX_NORM = 1.0
STEP_COUNT = 100
COLUMN_SPLIT = (True, False, True, False)

LAYERS = 32
DATA = 4
DEVICES = 16
ROWS = (64, 16, 64, 64)
COLS = (192, 256, 256, 256)
PACK = (144, 128, 0, 64)
PACKED = 192
SLOTS = 3
AHEAD = 6
GROUP = 8
CHUNKS = 4
MESH = pl.DeviceIdType.MESH


def grad_spec(col_split):
    return P("data", None, None, "model") if col_split else P("data", None, "model", None)


def state_spec(col_split):
    return P(None, "data", "model") if col_split else P(None, ("model", "data"), None)


def replica_spec(col_split):
    return P(None, None, "model") if col_split else P(None, "model", None)


def pack_layer(dst, qkv, proj, fcin, fcout):
    dst[0:64, :] = fcin.astype(jnp.bfloat16)
    dst[64:128, :] = fcout.astype(jnp.bfloat16)
    dst[128:144, :] = proj.astype(jnp.bfloat16)
    wide = qkv[:, 0:128].astype(jnp.bfloat16)
    thin = qkv[:, 128:192]
    dst[144:176, 0:128] = wide[0:32]
    dst[144:176, 128:256] = wide[32:64]
    left = jnp.concatenate([thin[0:16], thin[16:32]], axis=1)
    right = jnp.concatenate([thin[32:48], thin[48:64]], axis=1)
    dst[176:192, 0:128] = left.astype(jnp.bfloat16)
    dst[176:192, 128:256] = right.astype(jnp.bfloat16)


def column_sums(scr):
    folded = scr[:, 0:128] + scr[:, 128:256]
    return jnp.sum(jnp.transpose(folded), axis=0, keepdims=True)


def step_kernel(*refs):
    grads, weights, firsts, seconds = refs[0:4], refs[4:8], refs[8:12], refs[12:16]
    out_w, out_m, out_v = refs[16:20], refs[20:24], refs[24:28]
    out_b = refs[28 : 28 + CHUNKS]
    scr = refs[28 + CHUNKS :]
    stage, w_buf, m_buf, v_buf, u_buf = scr[0:4], scr[4:8], scr[8:12], scr[12:16], scr[16:20]
    snd, rcv, n_acc, wn_acc, un_acc, ratio, sync_src, sync_a, sync_b = scr[20:29]
    load_sem, state_sem, send_sem, recv_sem, sync_send, sync_recv, out_sem = scr[29:36]

    d = lax.axis_index("data")
    m = lax.axis_index("model")
    gid = m * DATA + d

    def coords(dev):
        return (dev // DATA, dev % DATA)

    def loads(layer, slot):
        return [pltpu.make_async_copy(grads[a].at[0, layer], stage[a].at[slot], load_sem.at[slot, a]) for a in range(4)]

    for layer in range(SLOTS):
        for copy in loads(layer, layer):
            copy.start()

    barrier = pltpu.get_barrier_semaphore()

    def greet(off, carry):
        pl.semaphore_signal(barrier, inc=1, device_id=coords((gid + off) % DEVICES), device_id_type=MESH)
        return carry

    lax.fori_loop(1, DEVICES, greet, 0)
    pl.semaphore_wait(barrier, DEVICES - 1)

    def exchange(layer, k):
        return pltpu.make_async_remote_copy(
            src_ref=snd.at[k - 1, layer],
            dst_ref=rcv.at[k, layer],
            send_sem=send_sem.at[k - 1, layer],
            recv_sem=recv_sem.at[k - 1, layer],
            device_id=(m, (d + k) % DATA),
            device_id_type=MESH,
        )

    def produce(layer):
        slot = lax.rem(layer, SLOTS)
        for copy in loads(layer, slot):
            copy.wait()
        for k in (2, 1, 3, 0):
            owner = (d + k) % DATA
            big = pl.ds(pl.multiple_of(owner * 64, 64), 64)
            small = pl.ds(pl.multiple_of(owner * 16, 16), 16)
            dst = snd.at[k - 1, layer] if k else rcv.at[0, layer]
            pack_layer(dst, stage[0][slot, big, :], stage[1][slot, small, :], stage[2][slot, big, :], stage[3][slot, big, :])
            if k:
                exchange(layer, k).start()

        @pl.when(layer + SLOTS < LAYERS)
        def _():
            for copy in loads(layer + SLOTS, slot):
                copy.start()

    def produce_loop(layer, carry):
        produce(layer)
        return carry

    lax.fori_loop(0, AHEAD, produce_loop, 0)

    state_copies = []
    for idx, (source, target) in enumerate(((weights, w_buf), (firsts, m_buf), (seconds, v_buf))):
        for a in range(4):
            copy = pltpu.make_async_copy(source[a], target[a], state_sem.at[idx, a])
            copy.start()
            state_copies.append(copy)
    n_acc[...] = jnp.zeros_like(n_acc)
    wn_acc[...] = jnp.zeros_like(wn_acc)
    un_acc[...] = jnp.zeros_like(un_acc)
    for copy in state_copies:
        copy.wait()

    def consume(layer, carry):
        @pl.when(layer + AHEAD < LAYERS)
        def _():
            produce(layer + AHEAD)

        for a in range(4):
            w = w_buf[a][layer]
            wn_acc[pl.ds(a * LAYERS + layer, 1), 0 : COLS[a]] = jnp.sum(w * w, axis=0, keepdims=True)
        for k in (1, 2, 3):
            exchange(layer, k).wait_recv()

        def gathered(first, rows, col=0, cols=256):
            parts = [rcv[k, layer, first : first + rows, col : col + cols].astype(jnp.float32) for k in range(4)]
            return (parts[0] + parts[1] + parts[2] + parts[3]) * (1.0 / DATA)

        def squares(x):
            rows, cols = x.shape
            return jnp.sum((x * x).reshape(rows // 8, 8, cols), axis=0)

        fcin = gathered(0, 64)
        u_buf[2][layer] = fcin
        fcout = gathered(64, 64)
        u_buf[3][layer] = fcout
        proj = gathered(128, 16)
        u_buf[1][layer] = proj
        wide = gathered(144, 32)
        u_buf[0][layer, 0:32, 0:128] = wide[:, 0:128]
        u_buf[0][layer, 32:64, 0:128] = wide[:, 128:256]
        thin = gathered(176, 16)
        for q in range(4):
            u_buf[0][layer, 16 * q : 16 * q + 16, 128:192] = thin[:, 64 * q : 64 * q + 64]
        n_acc[...] += squares(fcin) + squares(fcout) + squares(proj) + squares(wide) + squares(thin)
        return carry

    lax.fori_loop(0, LAYERS, consume, 0)

    row_idx = lax.broadcasted_iota(jnp.int32, (8, 128), 0)

    def share(sync, phase, tile):
        sync_src[phase] = tile
        sync[pl.ds(gid, 1)] = tile[None]

        def tile_copy(slot, dev):
            return pltpu.make_async_remote_copy(
                src_ref=sync_src.at[phase],
                dst_ref=sync.at[slot],
                send_sem=sync_send.at[phase, (dev - gid + DEVICES) % DEVICES],
                recv_sem=sync_recv.at[phase, slot],
                device_id=coords(dev),
                device_id_type=MESH,
            )

        def send(off, carry):
            tile_copy(gid, (gid + off) % DEVICES).start()
            return carry

        def receive(off, carry):
            dev = (gid + DEVICES - off) % DEVICES
            tile_copy(dev, dev).wait_recv()
            return carry

        def drain(off, carry):
            tile_copy(gid, (gid + off) % DEVICES).wait_send()
            return carry

        lax.fori_loop(1, DEVICES, send, 0)
        lax.fori_loop(1, DEVICES, receive, 0)
        lax.fori_loop(1, DEVICES, drain, 0)
        return jnp.sum(sync[...], axis=0)

    n_row = jnp.sum(n_acc[:, 0:128] + n_acc[:, 128:256], axis=0, keepdims=True)
    tile = jnp.where(row_idx == 0, n_row, jnp.where(row_idx == 1, column_sums(wn_acc), 0.0))
    totals = share(sync_a, 0, tile)
    weight_sq = totals[1:2, :]
    total_norm = jnp.sqrt(jnp.sum(totals[0:1, :], axis=1, keepdims=True))
    clip_coef = jnp.minimum(1.0, MAX_NORM / total_norm)

    def result_copy(source, target, a, group, idx):
        part = pl.ds(group * GROUP, GROUP)
        return pltpu.make_async_copy(source[a].at[part], target[a].at[part], out_sem.at[idx, a, group])

    def direction(layer, carry):
        for a in range(4):
            w = w_buf[a][layer]
            clipped = clip_coef * u_buf[a][layer]
            first = BETA_ONE * m_buf[a][layer] + (1.0 - BETA_ONE) * clipped
            second = BETA_TWO * v_buf[a][layer] + (1.0 - BETA_TWO) * clipped * clipped
            m_buf[a][layer] = first
            v_buf[a][layer] = second
            first_hat = first * (1.0 / (1.0 - BETA_ONE**STEP_COUNT))
            second_hat = second * (1.0 / (1.0 - BETA_TWO**STEP_COUNT))
            u = first_hat / (jnp.sqrt(second_hat) + ADAM_EPS) + DECAY_RATE * w
            u_buf[a][layer] = u
            un_acc[pl.ds(a * LAYERS + layer, 1), 0 : COLS[a]] = jnp.sum(u * u, axis=0, keepdims=True)

        @pl.when(lax.rem(layer, GROUP) == GROUP - 1)
        def _():
            for a in range(4):
                result_copy(m_buf, out_m, a, layer // GROUP, 0).start()
                result_copy(v_buf, out_v, a, layer // GROUP, 1).start()

        return carry

    lax.fori_loop(0, LAYERS, direction, 0)
    for k in (1, 2, 3):

        def sent(layer, carry):
            exchange(layer, k).wait_send()
            return carry

        lax.fori_loop(0, LAYERS, sent, 0)

    totals = share(sync_b, 1, jnp.where(row_idx == 0, column_sums(un_acc), 0.0))
    scaled = LEARN_RATE * (jnp.sqrt(weight_sq) / jnp.sqrt(totals[0:1, :]))
    spread = jnp.transpose(jnp.broadcast_to(scaled, (128, 128)))
    ratio[:, 0:128] = spread
    ratio[:, 128:256] = spread

    per_chunk = LAYERS // CHUNKS

    def replica_copy(group):
        return pltpu.make_async_copy(snd.at[0, pl.ds(group * per_chunk, per_chunk)], out_b[group], out_sem.at[3, 0, group])

    for group in range(CHUNKS):

        def finish(layer, carry):
            rows = []
            for a in range(4):
                factor = ratio[pl.ds(a * LAYERS + layer, 1), 0 : COLS[a]]
                w = w_buf[a][layer] - factor * u_buf[a][layer]
                w_buf[a][layer] = w
                rows.append(w)
            pack_layer(snd.at[0, layer], *rows)
            return carry

        lax.fori_loop(group * per_chunk, (group + 1) * per_chunk, finish, 0)
        replica_copy(group).start()
        for a in range(4):
            result_copy(w_buf, out_w, a, group, 2).start()

    for group in range(CHUNKS):
        replica_copy(group).wait()
        for a in range(4):
            result_copy(m_buf, out_m, a, group, 0).wait()
            result_copy(v_buf, out_v, a, group, 1).wait()
            result_copy(w_buf, out_w, a, group, 2).wait()


def run_step(arrays):
    grads, weights, firsts, seconds = (arrays[i::4] for i in range(4))
    state_shapes = [jax.ShapeDtypeStruct(w.shape, jnp.float32) for w in weights]
    pieces = [jax.ShapeDtypeStruct((LAYERS // CHUNKS, PACKED, 256), jnp.bfloat16)] * CHUNKS
    state_scratch = [pltpu.VMEM((LAYERS, ROWS[a], COLS[a]), jnp.float32) for a in range(4)]
    scratch = [pltpu.VMEM((SLOTS, g.shape[2], g.shape[3]), jnp.float32) for g in grads]
    scratch += state_scratch * 4
    scratch += [
        pltpu.VMEM((3, LAYERS, PACKED, 256), jnp.bfloat16),
        pltpu.VMEM((4, LAYERS, PACKED, 256), jnp.bfloat16),
        pltpu.VMEM((8, 256), jnp.float32),
        pltpu.VMEM((128, 256), jnp.float32),
        pltpu.VMEM((128, 256), jnp.float32),
        pltpu.VMEM((128, 256), jnp.float32),
        pltpu.VMEM((2, 8, 128), jnp.float32),
        pltpu.VMEM((DEVICES, 8, 128), jnp.float32),
        pltpu.VMEM((DEVICES, 8, 128), jnp.float32),
        pltpu.SemaphoreType.DMA((SLOTS, 4)),
        pltpu.SemaphoreType.DMA((3, 4)),
        pltpu.SemaphoreType.DMA((3, LAYERS)),
        pltpu.SemaphoreType.DMA((3, LAYERS)),
        pltpu.SemaphoreType.DMA((2, DEVICES)),
        pltpu.SemaphoreType.DMA((2, DEVICES)),
        pltpu.SemaphoreType.DMA((4, 4, LAYERS // GROUP)),
    ]
    anywhere = pl.BlockSpec(memory_space=pl.ANY)
    return pl.pallas_call(
        step_kernel,
        out_shape=state_shapes * 3 + pieces,
        in_specs=[anywhere] * 16,
        out_specs=[anywhere] * (12 + CHUNKS),
        scratch_shapes=scratch,
        compiler_params=pltpu.CompilerParams(collective_id=0, has_side_effects=True, vmem_limit_bytes=63 << 20),
        name="lamb_step",
    )(*grads, *weights, *firsts, *seconds)


def assemble_kernel(has_alias, *refs):
    shards = refs[0:4]
    qkv, proj, fcin, fcout = refs[4 + 4 * has_alias :]
    d = lax.axis_index("data")
    partner = d + 1 - 2 * (d % 2)
    owners = (d, (d + 2) % DATA, partner, (partner + 2) % DATA)
    for owner, shard in zip(owners, shards):
        big = pl.ds(pl.multiple_of(owner * 64, 64), 64)
        small = pl.ds(pl.multiple_of(owner * 16, 16), 16)
        fcin[:, big, :] = shard[:, 0:64, :]
        fcout[:, big, :] = shard[:, 64:128, :]
        proj[:, small, :] = shard[:, 128:144, :]
        for half in range(2):
            rows = pl.ds(pl.multiple_of(owner * 64 + 32 * half, 32), 32)
            qkv[:, rows, 0:128] = shard[:, 144:176, 128 * half : 128 * half + 128]
        for q in range(4):
            rows = pl.ds(pl.multiple_of(owner * 64 + 16 * q, 16), 16)
            qkv[:, rows, 128:192] = shard[:, 176:192, 64 * q : 64 * q + 64]


def assemble(chunk, shards, previous):
    block = 2
    per_chunk = LAYERS // CHUNKS
    shapes = [(LAYERS, 256, 192), (LAYERS, 64, 256), (LAYERS, 256, 256), (LAYERS, 256, 256)]
    first = chunk * per_chunk // block
    in_specs = [pl.BlockSpec((block, PACKED, 256), lambda i: (i, 0, 0))] * 4
    in_specs += [pl.BlockSpec(memory_space=pl.ANY)] * len(previous)
    return pl.pallas_call(
        functools.partial(assemble_kernel, bool(previous)),
        grid=(per_chunk // block,),
        out_shape=[jax.ShapeDtypeStruct(s, jnp.bfloat16) for s in shapes],
        in_specs=in_specs,
        out_specs=[pl.BlockSpec((block, s[1], s[2]), lambda i: (first + i, 0, 0)) for s in shapes],
        input_output_aliases={4 + i: i for i in range(len(previous))},
        cost_estimate=pl.CostEstimate(flops=4_000_000, bytes_accessed=6_000_000, transcendentals=0),
        compiler_params=pltpu.CompilerParams(vmem_limit_bytes=16 << 20),
        name="assemble",
    )(*shards, *previous)


def solution(mesh):
    in_specs = []
    for col_split in COLUMN_SPLIT:
        in_specs.extend([grad_spec(col_split), state_spec(col_split), state_spec(col_split), state_spec(col_split)])
    out_specs = tuple([replica_spec(col_split) for col_split in COLUMN_SPLIT] + [state_spec(col_split) for col_split in COLUMN_SPLIT] * 3)

    across = [(i, (i + 2) % DATA) for i in range(DATA)]
    on_chip = [(i, i + 1 - 2 * (i % 2)) for i in range(DATA)]

    def device_step(*arrays):
        results = run_step(arrays)
        states, pieces = results[:12], results[12:]
        replicas = ()
        for chunk, own in enumerate(pieces):
            far = lax.ppermute(own, "data", across)
            near = lax.ppermute(own, "data", on_chip)
            far_near = lax.ppermute(far, "data", on_chip)
            replicas = assemble(chunk, (own, far, near, far_near), tuple(replicas))
        return tuple(replicas) + tuple(states)

    return jax.shard_map(device_step, mesh=mesh, in_specs=tuple(in_specs), out_specs=out_specs, check_vma=False)
```

```python
import functools

import jax
import jax.numpy as jnp
from jax import lax
from jax.experimental import pallas as pl
from jax.experimental.pallas import tpu as pltpu
from jax.sharding import PartitionSpec as P


LEARN_RATE = 0.08
BETA_ONE = 0.9
BETA_TWO = 0.999
ADAM_EPS = 1e-6
DECAY_RATE = 0.01
MAX_NORM = 1.0
STEP_COUNT = 100
COLUMN_SPLIT = (True, False, True, False)

LAYERS = 32
DATA = 4
DEVICES = 16
ROWS = (64, 16, 64, 64)
COLS = (192, 256, 256, 256)
PACKED = 192
SLOTS = 3
AHEAD = 6
GROUP = 8
CHUNKS = (4, 10, 10, 6, 2)
HEAD = CHUNKS[0]
UPDATE_FLOPS = 2_000_000_000
ASSEMBLE_FLOPS = 40_000_000
FIRST_SCALE = 1.0 / (1.0 - BETA_ONE**STEP_COUNT)
SECOND_SCALE = 1.0 / (1.0 - BETA_TWO**STEP_COUNT)
MESH = pl.DeviceIdType.MESH


def grad_spec(col_split):
    return P("data", None, None, "model") if col_split else P("data", None, "model", None)


def state_spec(col_split):
    return P(None, "data", "model") if col_split else P(None, ("model", "data"), None)


def replica_spec(col_split):
    return P(None, None, "model") if col_split else P(None, "model", None)


def pack_rest(dst, proj, fcin, fcout):
    dst[0:64, :] = fcin.astype(jnp.bfloat16)
    dst[64:128, :] = fcout.astype(jnp.bfloat16)
    dst[128:144, :] = proj.astype(jnp.bfloat16)


def pack_grad(dst, qkv):
    wide = qkv[:, 0:128].astype(jnp.bfloat16)
    thin = qkv[:, 128:192]
    dst[144:176, 0:128] = wide[0:32]
    dst[144:176, 128:256] = wide[32:64]
    left = jnp.concatenate([thin[0:16], thin[16:32]], axis=1)
    right = jnp.concatenate([thin[32:48], thin[48:64]], axis=1)
    dst[176:192, 0:128] = left.astype(jnp.bfloat16)
    dst[176:192, 128:256] = right.astype(jnp.bfloat16)


def pack_turned(dst, qkv):
    turned = jnp.transpose(qkv)
    left = jnp.concatenate([turned[0:48], turned[96:144]], axis=1)
    right = jnp.concatenate([turned[48:96], turned[144:192]], axis=1)
    dst[144:192, 0:128] = left.astype(jnp.bfloat16)
    dst[144:192, 128:256] = right.astype(jnp.bfloat16)


def column_sums(scr):
    folded = scr[:, 0:128] + scr[:, 128:256]
    return jnp.sum(jnp.transpose(folded), axis=0, keepdims=True)


def step_kernel(*refs):
    grads, weights, firsts, seconds = refs[0:4], refs[4:8], refs[8:12], refs[12:16]
    out_g, out_coef, out_ratio, out_far = refs[16:20], refs[20], refs[21], refs[22]
    out_b = refs[23 : 23 + len(CHUNKS)]
    scr = refs[23 + len(CHUNKS) :]
    stage, w_buf, m_buf, v_buf, g_buf = scr[0:4], scr[4:8], scr[8:12], scr[12:16], scr[16:20]
    turned, snd, rcv, n_acc, wn_acc, un_acc, coef, ratio, sync_src, sync_buf = scr[20:30]
    load_sem, state_sem, send_sem, recv_sem, sync_send, sync_recv, far_sem, out_sem, grad_sem = scr[30:39]

    d = lax.axis_index("data")
    m = lax.axis_index("model")
    gid = m * DATA + d

    def coords(dev):
        return (dev // DATA, dev % DATA)

    def loads(layer, slot):
        return [pltpu.make_async_copy(grads[a].at[0, layer], stage[a].at[slot], load_sem.at[slot, a]) for a in range(4)]

    for layer in range(SLOTS):
        for copy in loads(layer, layer):
            copy.start()

    barrier = pltpu.get_barrier_semaphore()

    def greet(off, carry):
        pl.semaphore_signal(barrier, inc=1, device_id=coords((gid + off) % DEVICES), device_id_type=MESH)
        return carry

    lax.fori_loop(1, DEVICES, greet, 0)

    def exchange(layer, k):
        return pltpu.make_async_remote_copy(
            src_ref=snd.at[k - 1, layer],
            dst_ref=rcv.at[k, layer],
            send_sem=send_sem.at[k - 1, layer],
            recv_sem=recv_sem.at[k - 1, layer],
            device_id=(m, (d + k) % DATA),
            device_id_type=MESH,
        )

    def produce(layer, opening=False):
        slot = lax.rem(layer, SLOTS)
        for copy in loads(layer, slot):
            copy.wait()
        turned[...] = jnp.transpose(stage[0][slot])
        for k in (2, 1, 3, 0):
            owner = (d + k) % DATA
            big = pl.ds(pl.multiple_of(owner * 64, 64), 64)
            small = pl.ds(pl.multiple_of(owner * 16, 16), 16)
            dst = snd.at[k - 1, layer] if k else rcv.at[0, layer]
            pack_rest(dst, stage[1][slot, small, :], stage[2][slot, big, :], stage[3][slot, big, :])
            pack_grad(dst, turned[big, :])
            if k and not opening:
                exchange(layer, k).start()
        if opening:
            pl.semaphore_wait(barrier, DEVICES - 1)
            for k in (2, 1, 3):
                exchange(layer, k).start()

        @pl.when(layer + SLOTS < LAYERS)
        def _():
            for copy in loads(layer + SLOTS, slot):
                copy.start()

    def produce_loop(layer, carry):
        produce(layer)
        return carry

    produce(jnp.int32(0), opening=True)
    lax.fori_loop(1, AHEAD, produce_loop, 0)

    state_copies = []
    for idx, (source, target) in enumerate(((weights, w_buf), (firsts, m_buf), (seconds, v_buf))):
        for a in range(4):
            copy = pltpu.make_async_copy(source[a], target[a], state_sem.at[idx, a])
            copy.start()
            state_copies.append(copy)
    n_acc[...] = jnp.zeros_like(n_acc)
    wn_acc[...] = jnp.zeros_like(wn_acc)
    un_acc[...] = jnp.zeros_like(un_acc)
    for copy in state_copies:
        copy.wait()

    def grad_copy(a, group):
        part = pl.ds(group * GROUP, GROUP)
        return pltpu.make_async_copy(g_buf[a].at[part], out_g[a].at[part], grad_sem.at[a, group])

    def consume(layer, carry):
        @pl.when(layer + AHEAD < LAYERS)
        def _():
            produce(layer + AHEAD)

        for a in range(4):
            w = w_buf[a][layer]
            wn_acc[pl.ds(a * LAYERS + layer, 1), 0 : COLS[a]] = jnp.sum(w * w, axis=0, keepdims=True)
            m_buf[a][layer] = (BETA_ONE * FIRST_SCALE) * m_buf[a][layer]
            v_buf[a][layer] = (BETA_TWO * SECOND_SCALE) * v_buf[a][layer]
        for k in (1, 2, 3):
            exchange(layer, k).wait_recv()

        def gathered(first, rows):
            parts = [rcv[k, layer, first : first + rows, :].astype(jnp.float32) for k in range(4)]
            return (parts[0] + parts[1] + parts[2] + parts[3]) * (1.0 / DATA)

        def squares(x):
            rows, cols = x.shape
            return jnp.sum((x * x).reshape(rows // 8, 8, cols), axis=0)

        fcin = gathered(0, 64)
        g_buf[2][layer] = fcin
        fcout = gathered(64, 64)
        g_buf[3][layer] = fcout
        proj = gathered(128, 16)
        g_buf[1][layer] = proj
        wide = gathered(144, 32)
        g_buf[0][layer, 0:32, 0:128] = wide[:, 0:128]
        g_buf[0][layer, 32:64, 0:128] = wide[:, 128:256]
        thin = gathered(176, 16)
        for q in range(4):
            g_buf[0][layer, 16 * q : 16 * q + 16, 128:192] = thin[:, 64 * q : 64 * q + 64]
        n_acc[...] += squares(fcin) + squares(fcout) + squares(proj) + squares(wide) + squares(thin)

        @pl.when(lax.rem(layer, GROUP) == GROUP - 1)
        def _():
            for a in range(4):
                grad_copy(a, layer // GROUP).start()

        return carry

    lax.fori_loop(0, LAYERS, consume, 0)

    row_idx = lax.broadcasted_iota(jnp.int32, (8, 128), 0)

    def tile_copy(phase, slot, dev):
        return pltpu.make_async_remote_copy(
            src_ref=sync_src.at[phase],
            dst_ref=sync_buf.at[phase, slot],
            send_sem=sync_send.at[phase, (dev - gid + DEVICES) % DEVICES],
            recv_sem=sync_recv.at[phase, slot],
            device_id=coords(dev),
            device_id_type=MESH,
        )

    def share(phase, tile):
        sync_src[phase] = tile
        sync_buf[phase, pl.ds(gid, 1)] = tile[None]

        def send(off, carry):
            tile_copy(phase, gid, (gid + off) % DEVICES).start()
            return carry

        lax.fori_loop(1, DEVICES, send, 0)

    def collect(phase):
        def receive(off, carry):
            dev = (gid + DEVICES - off) % DEVICES
            tile_copy(phase, dev, dev).wait_recv()
            return carry

        lax.fori_loop(1, DEVICES, receive, 0)
        return jnp.sum(sync_buf[phase], axis=0)

    n_row = jnp.sum(n_acc[:, 0:128] + n_acc[:, 128:256], axis=0, keepdims=True)
    share(0, jnp.where(row_idx == 0, n_row, 0.0))
    share(1, jnp.where(row_idx == 0, column_sums(wn_acc), 0.0))
    total_norm = jnp.sqrt(jnp.sum(collect(0)[0:1, :], axis=1, keepdims=True))
    clip_coef = jnp.minimum(1.0, MAX_NORM / total_norm)
    coef[...] = jnp.broadcast_to(clip_coef, (8, 128))
    first_coef = ((1.0 - BETA_ONE) * FIRST_SCALE) * clip_coef
    second_coef = ((1.0 - BETA_TWO) * SECOND_SCALE) * clip_coef * clip_coef

    def direction(layer, carry):
        for a in range(4):
            g = g_buf[a][layer]
            first_hat = m_buf[a][layer] + first_coef * g
            second_hat = v_buf[a][layer] + second_coef * (g * g)
            u = first_hat / (jnp.sqrt(second_hat) + ADAM_EPS) + DECAY_RATE * w_buf[a][layer]
            m_buf[a][layer] = u
            un_acc[pl.ds(a * LAYERS + layer, 1), 0 : COLS[a]] = jnp.sum(u * u, axis=0, keepdims=True)
        return carry

    def set_ratio(weight_sq, update_sq):
        scaled = LEARN_RATE * (jnp.sqrt(weight_sq) / jnp.sqrt(update_sq))
        spread = jnp.transpose(jnp.broadcast_to(scaled, (128, 128)))
        ratio[:, 0:128] = spread
        ratio[:, 128:256] = spread

    def finish(layer, carry):
        rows = []
        for a in range(4):
            factor = ratio[pl.ds(a * LAYERS + layer, 1), 0 : COLS[a]]
            rows.append(w_buf[a][layer] - factor * m_buf[a][layer])
        pack_rest(snd.at[0, layer], *rows[1:])
        pack_turned(snd.at[0, layer], rows[0])
        return carry

    def sent(layer, carry):
        for k in (1, 2, 3):
            exchange(layer, k).wait_send()
        return carry

    starts = [sum(CHUNKS[:i]) for i in range(len(CHUNKS))]

    def replica_copy(i):
        return pltpu.make_async_copy(snd.at[0, pl.ds(starts[i], CHUNKS[i])], out_b[i], out_sem.at[i])

    far = pltpu.make_async_remote_copy(
        src_ref=snd.at[0, pl.ds(0, HEAD)],
        dst_ref=out_far,
        send_sem=far_sem.at[0],
        recv_sem=far_sem.at[1],
        device_id=(m, (d + 2) % DATA),
        device_id_type=MESH,
    )
    coef_copy = pltpu.make_async_copy(coef, out_coef, out_sem.at[len(CHUNKS)])
    ratio_copy = pltpu.make_async_copy(ratio, out_ratio, out_sem.at[len(CHUNKS) + 1])

    lane = lax.broadcasted_iota(jnp.int32, (1, 128), 1) % LAYERS
    lax.fori_loop(0, HEAD, direction, 0)
    share(2, jnp.where(row_idx == 0, column_sums(un_acc), 0.0))
    coef_copy.start()
    lax.fori_loop(0, LAYERS, sent, 0)
    lax.fori_loop(HEAD, LAYERS, direction, 0)
    share(3, jnp.where(row_idx == 0, column_sums(un_acc), 0.0))
    weight_sq = collect(1)[0:1, :]
    set_ratio(weight_sq, jnp.where(lane < HEAD, collect(2)[0:1, :], 1.0))
    lax.fori_loop(0, HEAD, finish, 0)
    far.start()
    replica_copy(0).start()
    set_ratio(weight_sq, collect(3)[0:1, :])
    ratio_copy.start()
    for i in range(1, len(CHUNKS)):
        lax.fori_loop(starts[i], starts[i] + CHUNKS[i], finish, 0)
        replica_copy(i).start()

    def drain(off, carry):
        for phase in range(4):
            tile_copy(phase, gid, (gid + off) % DEVICES).wait_send()
        return carry

    lax.fori_loop(1, DEVICES, drain, 0)
    coef_copy.wait()
    ratio_copy.wait()
    for group in range(LAYERS // GROUP):
        for a in range(4):
            grad_copy(a, group).wait()
    for i in range(len(CHUNKS)):
        replica_copy(i).wait()
    far.wait()


def run_step(grads, weights, firsts, seconds):
    state_shapes = [jax.ShapeDtypeStruct(w.shape, jnp.float32) for w in weights]
    pieces = [jax.ShapeDtypeStruct((n, PACKED, 256), jnp.bfloat16) for n in CHUNKS]
    small = [jax.ShapeDtypeStruct((8, 128), jnp.float32), jax.ShapeDtypeStruct((128, 256), jnp.float32)]
    state_scratch = [pltpu.VMEM((LAYERS, ROWS[a], COLS[a]), jnp.float32) for a in range(4)]
    scratch = [pltpu.VMEM((SLOTS, g.shape[2], g.shape[3]), jnp.float32) for g in grads]
    scratch += state_scratch * 4
    scratch += [
        pltpu.VMEM((256, 192), jnp.float32),
        pltpu.VMEM((3, LAYERS, PACKED, 256), jnp.bfloat16),
        pltpu.VMEM((4, LAYERS, PACKED, 256), jnp.bfloat16),
        pltpu.VMEM((8, 256), jnp.float32),
        pltpu.VMEM((128, 256), jnp.float32),
        pltpu.VMEM((128, 256), jnp.float32),
        pltpu.VMEM((8, 128), jnp.float32),
        pltpu.VMEM((128, 256), jnp.float32),
        pltpu.VMEM((4, 8, 128), jnp.float32),
        pltpu.VMEM((4, DEVICES, 8, 128), jnp.float32),
        pltpu.SemaphoreType.DMA((SLOTS, 4)),
        pltpu.SemaphoreType.DMA((3, 4)),
        pltpu.SemaphoreType.DMA((3, LAYERS)),
        pltpu.SemaphoreType.DMA((3, LAYERS)),
        pltpu.SemaphoreType.DMA((4, DEVICES)),
        pltpu.SemaphoreType.DMA((4, DEVICES)),
        pltpu.SemaphoreType.DMA((2,)),
        pltpu.SemaphoreType.DMA((len(CHUNKS) + 2,)),
        pltpu.SemaphoreType.DMA((4, LAYERS // GROUP)),
    ]
    anywhere = pl.BlockSpec(memory_space=pl.ANY)
    out_shape = state_shapes + small + pieces[:1] + pieces
    results = pl.pallas_call(
        step_kernel,
        out_shape=out_shape,
        in_specs=[anywhere] * 16,
        out_specs=[anywhere] * len(out_shape),
        scratch_shapes=scratch,
        compiler_params=pltpu.CompilerParams(collective_id=0, has_side_effects=True, vmem_limit_bytes=63 << 20),
        name="lamb_step",
    )(*grads, *weights, *firsts, *seconds)
    return results[0:4], results[4], results[5], results[6], results[7:]


def update_kernel(*refs):
    coef, ratio = refs[0], refs[1]
    means, weights, firsts, seconds = refs[2:6], refs[6:10], refs[10:14], refs[14:18]
    out_w, out_m, out_v = refs[18:22], refs[22:26], refs[26:30]
    clip_coef = coef[0:1, 0:1]
    block = means[0].shape[0]
    for b in range(block):
        layer = pl.program_id(0) * block + b
        for a in range(4):
            w = weights[a][b]
            clipped = clip_coef * means[a][b]
            first = BETA_ONE * firsts[a][b] + (1.0 - BETA_ONE) * clipped
            second = BETA_TWO * seconds[a][b] + (1.0 - BETA_TWO) * clipped * clipped
            out_m[a][b] = first
            out_v[a][b] = second
            u = (first * FIRST_SCALE) / (jnp.sqrt(second * SECOND_SCALE) + ADAM_EPS) + DECAY_RATE * w
            out_w[a][b] = w - ratio[pl.ds(a * LAYERS + layer, 1), 0 : COLS[a]] * u


def update(coef, ratio, means, weights, firsts, seconds):
    block = 2
    layer_specs = [pl.BlockSpec((block, ROWS[a], COLS[a]), lambda i: (i, 0, 0)) for a in range(4)]
    return pl.pallas_call(
        update_kernel,
        grid=(LAYERS // block,),
        out_shape=[jax.ShapeDtypeStruct(w.shape, jnp.float32) for w in weights] * 3,
        in_specs=[pl.BlockSpec((8, 128), lambda i: (0, 0)), pl.BlockSpec((128, 256), lambda i: (0, 0))] + layer_specs * 4,
        out_specs=layer_specs * 3,
        cost_estimate=pl.CostEstimate(flops=UPDATE_FLOPS, bytes_accessed=47_000_000, transcendentals=0),
        compiler_params=pltpu.CompilerParams(vmem_limit_bytes=60 << 20),
        name="update",
    )(coef, ratio, *means, *weights, *firsts, *seconds)


def assemble_kernel(has_alias, *refs):
    shards = refs[0:4]
    qkv, proj, fcin, fcout, parts = refs[4 + 4 * has_alias :]
    d = lax.axis_index("data")
    partner = d + 1 - 2 * (d % 2)
    owners = (d, (d + 2) % DATA, partner, (partner + 2) % DATA)
    for owner, shard in zip(owners, shards):
        big = pl.ds(pl.multiple_of(owner * 64, 64), 64)
        small = pl.ds(pl.multiple_of(owner * 16, 16), 16)
        fcin[:, big, :] = shard[:, 0:64, :]
        fcout[:, big, :] = shard[:, 64:128, :]
        proj[:, small, :] = shard[:, 128:144, :]
        parts[owner] = shard[:, 144:192, :]
    for half in range(2):
        first, second = parts[2 * half], parts[2 * half + 1]
        for q, lane in ((0, 0), (48, 128), (96, 64), (144, 192)):
            pair = jnp.concatenate([first[:, :, lane : lane + 64], second[:, :, lane : lane + 64]], axis=2)
            qkv[:, q : q + 48, 128 * half : 128 * half + 128] = pair


def assemble(chunk, shards, previous):
    block = 2
    shapes = [(LAYERS, 192, 256), (LAYERS, 64, 256), (LAYERS, 256, 256), (LAYERS, 256, 256)]
    first = sum(CHUNKS[:chunk]) // block
    in_specs = [pl.BlockSpec((block, PACKED, 256), lambda i: (i, 0, 0))] * 4
    in_specs += [pl.BlockSpec(memory_space=pl.ANY)] * len(previous)
    return pl.pallas_call(
        functools.partial(assemble_kernel, bool(previous)),
        grid=(CHUNKS[chunk] // block,),
        out_shape=[jax.ShapeDtypeStruct(s, jnp.bfloat16) for s in shapes],
        in_specs=in_specs,
        out_specs=[pl.BlockSpec((block, s[1], s[2]), lambda i: (first + i, 0, 0)) for s in shapes],
        scratch_shapes=[pltpu.VMEM((4, block, 48, 256), jnp.bfloat16)],
        input_output_aliases={4 + i: i for i in range(len(previous))},
        cost_estimate=pl.CostEstimate(flops=ASSEMBLE_FLOPS * CHUNKS[chunk], bytes_accessed=800_000 * CHUNKS[chunk], transcendentals=0),
        compiler_params=pltpu.CompilerParams(vmem_limit_bytes=24 << 20),
        name="assemble",
    )(*shards, *previous)


def solution(mesh):
    in_specs = []
    for col_split in COLUMN_SPLIT:
        in_specs.extend([grad_spec(col_split), state_spec(col_split), state_spec(col_split), state_spec(col_split)])
    out_specs = tuple([replica_spec(col_split) for col_split in COLUMN_SPLIT] + [state_spec(col_split) for col_split in COLUMN_SPLIT] * 3)

    across = [(i, (i + 2) % DATA) for i in range(DATA)]
    on_chip = [(i, i + 1 - 2 * (i % 2)) for i in range(DATA)]

    def device_step(*arrays):
        grads, weights, firsts, seconds = (arrays[i::4] for i in range(4))
        grads = (jnp.swapaxes(grads[0], 2, 3), *grads[1:])
        means, coef, ratio, far_head, pieces = run_step(grads, weights, firsts, seconds)
        states = update(coef, ratio, means, weights, firsts, seconds)
        replicas = ()
        for chunk, own in enumerate(pieces):
            far = lax.ppermute(own, "data", across) if chunk else far_head
            near = lax.ppermute(own, "data", on_chip)
            far_near = lax.ppermute(far, "data", on_chip)
            replicas = assemble(chunk, (own, far, near, far_near), tuple(replicas))
        return (jnp.swapaxes(replicas[0], 1, 2), *replicas[1:], *states)

    return jax.shard_map(device_step, mesh=mesh, in_specs=tuple(in_specs), out_specs=out_specs, check_vma=False)
```

```python
import functools

import jax
import jax.numpy as jnp
from jax import lax
from jax.experimental import pallas as pl
from jax.experimental.pallas import tpu as pltpu
from jax.sharding import PartitionSpec as P


LEARN_RATE = 0.08
BETA_ONE = 0.9
BETA_TWO = 0.999
ADAM_EPS = 1e-6
DECAY_RATE = 0.01
MAX_NORM = 1.0
STEP_COUNT = 100
COLUMN_SPLIT = (True, False, True, False)

LAYERS = 32
DATA = 4
DEVICES = 16
ROWS = (64, 16, 64, 64)
COLS = (192, 256, 256, 256)
KINDS = 4
LANES = 128
WIDE = 256
THIRD = 48
PACKED = 192
PHASES = 4
SLOTS = 3
AHEAD = 6
GROUP = 8
CHUNKS = (6, 10, 10, 4, 2)
HEAD = CHUNKS[0]
LATE = 1
UPDATE_FLOPS = 2_000_000_000
ASSEMBLE_FLOPS = 40_000_000
FIRST_SCALE = 1.0 / (1.0 - BETA_ONE**STEP_COUNT)
SECOND_SCALE = 1.0 / (1.0 - BETA_TWO**STEP_COUNT)
MESH = pl.DeviceIdType.MESH


def grad_spec(col_split):
    return P("data", None, None, "model") if col_split else P("data", None, "model", None)


def state_spec(col_split):
    return P(None, "data", "model") if col_split else P(None, ("model", "data"), None)


def replica_spec(col_split):
    return P(None, None, "model") if col_split else P(None, "model", None)


def split(refs, *sizes):
    groups, start = [], 0
    for size in sizes:
        groups.append(refs[start] if size is None else refs[start : start + size])
        start += 1 if size is None else size
    return groups


def pack_rest(dst, proj, fcin, fcout):
    start = 0
    for rows in (fcin, fcout, proj):
        dst[start : start + rows.shape[0], :] = rows.astype(jnp.bfloat16)
        start += rows.shape[0]


def pack_grad(dst, qkv):
    for half in range(2):
        side = slice(half * LANES, half * LANES + LANES)
        first = half * 32
        dst[144:176, side] = qkv[first : first + 32, :LANES].astype(jnp.bfloat16)
        thin = qkv[first : first + 32, LANES:]
        dst[176:192, side] = jnp.concatenate([thin[:16], thin[16:]], axis=1).astype(jnp.bfloat16)


def pack_turned(dst, qkv):
    turned = jnp.transpose(qkv)
    blocks = [turned[THIRD * q : THIRD * (q + 1)] for q in range(4)]
    for half in range(2):
        side = slice(half * LANES, half * LANES + LANES)
        dst[144:192, side] = jnp.concatenate([blocks[half], blocks[half + 2]], axis=1).astype(jnp.bfloat16)


def column_sums(scr):
    folded = scr[:, :LANES] + scr[:, LANES:]
    return jnp.sum(jnp.transpose(folded), axis=0, keepdims=True)


def step_kernel(*refs):
    operands, out_g, (out_coef, out_ratio, out_far), out_b, buffers, singles, sems = split(
        refs, KINDS * 4, KINDS, 3, len(CHUNKS), KINDS * 5, 10, 9
    )
    grads, weights, firsts, seconds = split(operands, *[KINDS] * 4)
    stage, w_buf, m_buf, v_buf, g_buf = split(buffers, *[KINDS] * 5)
    turned, snd, rcv, n_acc, wn_acc, un_acc, coef, ratio, sync_src, sync_buf = singles
    load_sem, state_sem, send_sem, recv_sem, sync_send, sync_recv, far_sem, out_sem, grad_sem = sems

    d = lax.axis_index("data")
    m = lax.axis_index("model")
    gid = m * DATA + d

    def coords(dev):
        return (dev // DATA, dev % DATA)

    def loads(layer, slot):
        return [pltpu.make_async_copy(grads[a].at[0, layer], stage[a].at[slot], load_sem.at[slot, a]) for a in range(KINDS)]

    for layer in range(SLOTS):
        for copy in loads(layer, layer):
            copy.start()

    barrier = pltpu.get_barrier_semaphore()

    def greet(off, carry):
        pl.semaphore_signal(barrier, inc=1, device_id=coords((gid + off) % DEVICES), device_id_type=MESH)
        return carry

    lax.fori_loop(1, DEVICES, greet, 0)

    def exchange(layer, k):
        return pltpu.make_async_remote_copy(
            src_ref=snd.at[k - 1, layer],
            dst_ref=rcv.at[k, layer],
            send_sem=send_sem.at[k - 1, layer],
            recv_sem=recv_sem.at[k - 1, layer],
            device_id=(m, (d + k) % DATA),
            device_id_type=MESH,
        )

    def produce(layer, opening=False):
        slot = lax.rem(layer, SLOTS)
        for copy in loads(layer, slot):
            copy.wait()
        turned[...] = jnp.transpose(stage[0][slot])
        for k in (2, 1, 3, 0):
            owner = (d + k) % DATA
            big = pl.ds(pl.multiple_of(owner * 64, 64), 64)
            small = pl.ds(pl.multiple_of(owner * 16, 16), 16)
            dst = snd.at[k - 1, layer] if k else rcv.at[0, layer]
            pack_rest(dst, stage[1][slot, small, :], stage[2][slot, big, :], stage[3][slot, big, :])
            pack_grad(dst, turned[big, :])
            if k and not opening:
                exchange(layer, k).start()
        if opening:
            pl.semaphore_wait(barrier, DEVICES - 1)
            for k in (2, 1, 3):
                exchange(layer, k).start()

        @pl.when(layer + SLOTS < LAYERS)
        def _():
            for copy in loads(layer + SLOTS, slot):
                copy.start()

    def produce_loop(layer, carry):
        produce(layer)
        return carry

    produce(jnp.int32(0), opening=True)
    lax.fori_loop(1, AHEAD, produce_loop, 0)

    state_copies = []
    for idx, (source, target) in enumerate(((weights, w_buf), (firsts, m_buf), (seconds, v_buf))):
        for a in range(KINDS):
            copy = pltpu.make_async_copy(source[a], target[a], state_sem.at[idx, a])
            copy.start()
            state_copies.append(copy)
    n_acc[...] = jnp.zeros_like(n_acc)
    wn_acc[...] = jnp.zeros_like(wn_acc)
    un_acc[...] = jnp.zeros_like(un_acc)
    for copy in state_copies:
        copy.wait()

    def grad_copy(a, group):
        part = pl.ds(group * GROUP, GROUP)
        return pltpu.make_async_copy(g_buf[a].at[part], out_g[a].at[part], grad_sem.at[a, group])

    def consume(layer, carry):
        @pl.when(layer + AHEAD < LAYERS)
        def _():
            produce(layer + AHEAD)

        for a in range(KINDS):
            w = w_buf[a][layer]
            wn_acc[pl.ds(a * LAYERS + layer, 1), 0 : COLS[a]] = jnp.sum(w * w, axis=0, keepdims=True)
            m_buf[a][layer] = (BETA_ONE * FIRST_SCALE) * m_buf[a][layer]
            v_buf[a][layer] = (BETA_TWO * SECOND_SCALE) * v_buf[a][layer]
        for k in (1, 2, 3):
            exchange(layer, k).wait_recv()

        def gathered(first, rows):
            parts = [rcv[k, layer, first : first + rows, :].astype(jnp.float32) for k in range(4)]
            return (parts[0] + parts[1] + parts[2] + parts[3]) * (1.0 / DATA)

        def squares(x):
            rows, cols = x.shape
            return jnp.sum((x * x).reshape(rows // 8, 8, cols), axis=0)

        fcin = gathered(0, 64)
        g_buf[2][layer] = fcin
        fcout = gathered(64, 64)
        g_buf[3][layer] = fcout
        proj = gathered(128, 16)
        g_buf[1][layer] = proj
        wide = gathered(144, 32)
        for half in range(2):
            g_buf[0][layer, 32 * half : 32 * half + 32, :LANES] = wide[:, LANES * half : LANES * half + LANES]
        thin = gathered(176, 16)
        for q in range(4):
            g_buf[0][layer, 16 * q : 16 * q + 16, LANES:] = thin[:, 64 * q : 64 * q + 64]
        n_acc[...] += squares(fcin) + squares(fcout) + squares(proj) + squares(wide) + squares(thin)

        @pl.when(lax.rem(layer, GROUP) == GROUP - 1)
        def _():
            for a in range(KINDS):
                grad_copy(a, layer // GROUP).start()

        return carry

    lax.fori_loop(0, LAYERS, consume, 0)

    def tile_copy(phase, slot, dev):
        return pltpu.make_async_remote_copy(
            src_ref=sync_src.at[phase],
            dst_ref=sync_buf.at[phase, slot],
            send_sem=sync_send.at[phase, (dev - gid + DEVICES) % DEVICES],
            recv_sem=sync_recv.at[phase, slot],
            device_id=coords(dev),
            device_id_type=MESH,
        )

    def share(phase, tile):
        sync_src[phase] = tile
        sync_buf[phase, pl.ds(gid, 1)] = tile[None]

        def send(off, carry):
            tile_copy(phase, gid, (gid + off) % DEVICES).start()
            return carry

        lax.fori_loop(1, DEVICES, send, 0)

    def collect(phase):
        def receive(off, carry):
            dev = (gid + DEVICES - off) % DEVICES
            tile_copy(phase, dev, dev).wait_recv()
            return carry

        lax.fori_loop(1, DEVICES, receive, 0)
        return jnp.sum(sync_buf[phase], axis=0)

    share(0, jnp.sum(n_acc[:, :LANES] + n_acc[:, LANES:], axis=0, keepdims=True))
    share(1, column_sums(wn_acc))
    total_norm = jnp.sqrt(jnp.sum(collect(0), axis=1, keepdims=True))
    clip_coef = jnp.minimum(1.0, MAX_NORM / total_norm)
    coef[...] = jnp.broadcast_to(clip_coef, coef.shape)
    first_coef = ((1.0 - BETA_ONE) * FIRST_SCALE) * clip_coef
    second_coef = ((1.0 - BETA_TWO) * SECOND_SCALE) * clip_coef * clip_coef

    def direction(layer, carry):
        for a in range(KINDS):
            g = g_buf[a][layer]
            first_hat = m_buf[a][layer] + first_coef * g
            second_hat = v_buf[a][layer] + second_coef * (g * g)
            u = first_hat / (jnp.sqrt(second_hat) + ADAM_EPS) + DECAY_RATE * w_buf[a][layer]
            m_buf[a][layer] = u
            un_acc[pl.ds(a * LAYERS + layer, 1), 0 : COLS[a]] = jnp.sum(u * u, axis=0, keepdims=True)
        return carry

    def set_ratio(weight_sq, update_sq):
        scaled = LEARN_RATE * (jnp.sqrt(weight_sq) / jnp.sqrt(update_sq))
        spread = jnp.transpose(jnp.broadcast_to(scaled, (LANES, LANES)))
        ratio[:, :LANES] = spread
        ratio[:, LANES:] = spread

    def finish(layer, carry):
        rows = []
        for a in range(KINDS):
            factor = ratio[pl.ds(a * LAYERS + layer, 1), 0 : COLS[a]]
            rows.append(w_buf[a][layer] - factor * m_buf[a][layer])
        pack_rest(snd.at[0, layer], *rows[1:])
        pack_turned(snd.at[0, layer], rows[0])
        return carry

    def sent(layer, carry):
        for k in (1, 2, 3):
            exchange(layer, k).wait_send()
        return carry

    starts = [sum(CHUNKS[:i]) for i in range(len(CHUNKS))]

    def replica_copy(i):
        return pltpu.make_async_copy(snd.at[0, pl.ds(starts[i], CHUNKS[i])], out_b[i], out_sem.at[i])

    def far(layer):
        return pltpu.make_async_remote_copy(
            src_ref=snd.at[0, layer],
            dst_ref=out_far.at[layer],
            send_sem=far_sem.at[0, layer],
            recv_sem=far_sem.at[1, layer],
            device_id=(m, (d + 2) % DATA),
            device_id_type=MESH,
        )

    def finish_and_send(layer, carry):
        finish(layer, carry)

        @pl.when(d % 2 == 1)
        def _():
            far(layer).start()

        return carry

    def send_late(layer, carry):
        @pl.when(d % 2 == 0)
        def _():
            far(layer).start()

        return carry

    def far_done(layer, carry):
        far(layer).wait()
        return carry

    coef_copy = pltpu.make_async_copy(coef, out_coef, out_sem.at[len(CHUNKS)])
    ratio_copy = pltpu.make_async_copy(ratio, out_ratio, out_sem.at[len(CHUNKS) + 1])

    lane = lax.broadcasted_iota(jnp.int32, (1, LANES), 1) % LAYERS
    lax.fori_loop(0, HEAD, direction, 0)
    share(2, column_sums(un_acc))
    coef_copy.start()
    lax.fori_loop(0, LAYERS, sent, 0)
    lax.fori_loop(HEAD, LAYERS, direction, 0)
    share(3, column_sums(un_acc))
    weight_sq = collect(1)
    set_ratio(weight_sq, jnp.where(lane < HEAD, collect(2), 1.0))
    lax.fori_loop(0, HEAD, finish_and_send, 0)
    replica_copy(0).start()
    set_ratio(weight_sq, collect(3))
    ratio_copy.start()
    for i in range(1, len(CHUNKS)):
        lax.fori_loop(starts[i], starts[i] + CHUNKS[i], finish, 0)
        replica_copy(i).start()
        if i == LATE:
            lax.fori_loop(0, HEAD, send_late, 0)

    def drain(off, carry):
        for phase in range(PHASES):
            tile_copy(phase, gid, (gid + off) % DEVICES).wait_send()
        return carry

    lax.fori_loop(1, DEVICES, drain, 0)
    coef_copy.wait()
    ratio_copy.wait()
    for group in range(LAYERS // GROUP):
        for a in range(KINDS):
            grad_copy(a, group).wait()
    for i in range(len(CHUNKS)):
        replica_copy(i).wait()
    lax.fori_loop(0, HEAD, far_done, 0)


def run_step(grads, weights, firsts, seconds):
    state_shapes = [jax.ShapeDtypeStruct(w.shape, jnp.float32) for w in weights]
    pieces = [jax.ShapeDtypeStruct((n, PACKED, 256), jnp.bfloat16) for n in CHUNKS]
    row = (1, LANES)
    table = (LANES, WIDE)
    small = [jax.ShapeDtypeStruct(shape, jnp.float32) for shape in (row, table)]
    scratch = [pltpu.VMEM((SLOTS, *g.shape[2:]), jnp.float32) for g in grads]
    scratch += [pltpu.VMEM((LAYERS, ROWS[a], COLS[a]), jnp.float32) for a in range(KINDS)] * 4
    scratch += [pltpu.VMEM((WIDE, COLS[0]), jnp.float32)]
    scratch += [pltpu.VMEM((n, LAYERS, PACKED, WIDE), jnp.bfloat16) for n in (DATA - 1, DATA)]
    shapes = [(8, WIDE), table, table, row, table, (PHASES, *row), (PHASES, DEVICES, *row)]
    scratch += [pltpu.VMEM(shape, jnp.float32) for shape in shapes]
    exchange_shape = (DATA - 1, LAYERS)
    sync_shape = (PHASES, DEVICES)
    shapes = [(SLOTS, KINDS), (3, KINDS), exchange_shape, exchange_shape, sync_shape, sync_shape]
    shapes += [(2, HEAD), (len(CHUNKS) + 2,), (KINDS, LAYERS // GROUP)]
    scratch += [pltpu.SemaphoreType.DMA(shape) for shape in shapes]
    anywhere = pl.BlockSpec(memory_space=pl.ANY)
    out_shape = state_shapes + small + [pieces[0]] + pieces
    results = pl.pallas_call(
        step_kernel,
        out_shape=out_shape,
        in_specs=[anywhere] * (KINDS * 4),
        out_specs=[anywhere] * len(out_shape),
        scratch_shapes=scratch,
        compiler_params=pltpu.CompilerParams(collective_id=0, has_side_effects=True, vmem_limit_bytes=63 << 20),
        name="lamb_step",
    )(*grads, *weights, *firsts, *seconds)
    return split(results, KINDS, None, None, None, len(CHUNKS))


def update_kernel(*refs):
    coef, ratio, means, weights, firsts, seconds, out_w, out_m, out_v = split(refs, None, None, *[KINDS] * 7)
    clip_coef = coef[:, :1]
    block = means[0].shape[0]
    for b in range(block):
        layer = pl.program_id(0) * block + b
        for a in range(KINDS):
            w = weights[a][b]
            clipped = clip_coef * means[a][b]
            first = BETA_ONE * firsts[a][b] + (1.0 - BETA_ONE) * clipped
            second = BETA_TWO * seconds[a][b] + (1.0 - BETA_TWO) * clipped * clipped
            out_m[a][b] = first
            out_v[a][b] = second
            u = (first * FIRST_SCALE) / (jnp.sqrt(second * SECOND_SCALE) + ADAM_EPS) + DECAY_RATE * w
            out_w[a][b] = w - ratio[pl.ds(a * LAYERS + layer, 1), 0 : COLS[a]] * u


def update(coef, ratio, means, weights, firsts, seconds):
    block = 2
    layer_specs = [pl.BlockSpec((block, ROWS[a], COLS[a]), lambda i: (i, 0, 0)) for a in range(KINDS)]
    return pl.pallas_call(
        update_kernel,
        grid=(LAYERS // block,),
        out_shape=[jax.ShapeDtypeStruct(w.shape, jnp.float32) for w in weights] * 3,
        in_specs=[pl.BlockSpec(table.shape, lambda i: (0, 0)) for table in (coef, ratio)] + layer_specs * 4,
        out_specs=layer_specs * 3,
        cost_estimate=pl.CostEstimate(flops=UPDATE_FLOPS, bytes_accessed=47_000_000, transcendentals=0),
        compiler_params=pltpu.CompilerParams(vmem_limit_bytes=60 << 20),
        name="update",
    )(coef, ratio, *means, *weights, *firsts, *seconds)


def assemble_kernel(has_alias, *refs):
    shards, _, (qkv, proj, fcin, fcout), parts = split(refs, DATA, KINDS * has_alias, KINDS, None)
    d = lax.axis_index("data")
    partner = d + 1 - 2 * (d % 2)
    owners = (d, (d + 2) % DATA, partner, (partner + 2) % DATA)
    for owner, shard in zip(owners, shards):
        big = pl.ds(pl.multiple_of(owner * 64, 64), 64)
        small = pl.ds(pl.multiple_of(owner * 16, 16), 16)
        fcin[:, big, :] = shard[:, 0:64, :]
        fcout[:, big, :] = shard[:, 64:128, :]
        proj[:, small, :] = shard[:, 128:144, :]
        parts[owner] = shard[:, 144:192, :]
    for half in range(2):
        side = slice(half * LANES, half * LANES + LANES)
        first, second = parts[2 * half], parts[2 * half + 1]
        for q in range(4):
            lane = (q % 2) * LANES + (q // 2) * 64
            pair = jnp.concatenate([shard[:, :, lane : lane + 64] for shard in (first, second)], axis=2)
            qkv[:, THIRD * q : THIRD * (q + 1), side] = pair


def assemble(chunk, shards, previous):
    block = 2
    shapes = [(LAYERS, 192, 256), (LAYERS, 64, 256), (LAYERS, 256, 256), (LAYERS, 256, 256)]
    first = sum(CHUNKS[:chunk]) // block
    in_specs = [pl.BlockSpec((block, PACKED, 256), lambda i: (i, 0, 0))] * 4
    in_specs += [pl.BlockSpec(memory_space=pl.ANY)] * len(previous)
    return pl.pallas_call(
        functools.partial(assemble_kernel, bool(previous)),
        grid=(CHUNKS[chunk] // block,),
        out_shape=[jax.ShapeDtypeStruct(s, jnp.bfloat16) for s in shapes],
        in_specs=in_specs,
        out_specs=[pl.BlockSpec((block, s[1], s[2]), lambda i: (first + i, 0, 0)) for s in shapes],
        scratch_shapes=[pltpu.VMEM((4, block, 48, 256), jnp.bfloat16)],
        input_output_aliases={4 + i: i for i in range(len(previous))},
        cost_estimate=pl.CostEstimate(flops=ASSEMBLE_FLOPS * CHUNKS[chunk], bytes_accessed=800_000 * CHUNKS[chunk], transcendentals=0),
        compiler_params=pltpu.CompilerParams(vmem_limit_bytes=24 << 20),
        name="assemble",
    )(*shards, *previous)


def solution(mesh):
    in_specs = []
    for col_split in COLUMN_SPLIT:
        in_specs.extend([grad_spec(col_split), state_spec(col_split), state_spec(col_split), state_spec(col_split)])
    out_specs = tuple([replica_spec(col_split) for col_split in COLUMN_SPLIT] + [state_spec(col_split) for col_split in COLUMN_SPLIT] * 3)

    across = [(i, (i + 2) % DATA) for i in range(DATA)]
    on_chip = [(i, i + 1 - 2 * (i % 2)) for i in range(DATA)]

    def device_step(*arrays):
        grads, weights, firsts, seconds = (arrays[i::4] for i in range(4))
        grads = (jnp.swapaxes(grads[0], 2, 3), *grads[1:])
        means, coef, ratio, far_head, pieces = run_step(grads, weights, firsts, seconds)
        states = update(coef, ratio, means, weights, firsts, seconds)
        replicas = ()
        for chunk, own in enumerate(pieces):
            far = lax.ppermute(own, "data", across) if chunk else far_head
            near = lax.ppermute(own, "data", on_chip)
            far_near = lax.ppermute(far, "data", on_chip)
            replicas = assemble(chunk, (own, far, near, far_near), tuple(replicas))
        return (jnp.swapaxes(replicas[0], 1, 2), *replicas[1:], *states)

    return jax.shard_map(device_step, mesh=mesh, in_specs=tuple(in_specs), out_specs=out_specs, check_vma=False)
```

```python
import functools

import jax
import jax.numpy as jnp
from jax import lax
from jax.experimental import pallas as pl
from jax.experimental.pallas import tpu as pltpu
from jax.sharding import PartitionSpec as P


LEARN_RATE = 0.08
BETA_ONE = 0.9
BETA_TWO = 0.999
ADAM_EPS = 1e-6
DECAY_RATE = 0.01
MAX_NORM = 1.0
STEP_COUNT = 100
COLUMN_SPLIT = (True, False, True, False)

LAYERS = 32
DATA = 4
DEVICES = 16
ROWS = (64, 16, 64, 64)
COLS = (192, 256, 256, 256)
KINDS = 4
LANES = 128
WIDE = 256
THIRD = 48
PACKED = 192
PHASES = 4
SLOTS = 3
AHEAD = 6
GROUP = 8
CHUNKS = (6, 10, 10, 4, 2)
HEAD = CHUNKS[0]
UPDATE_FLOPS = 2_000_000_000
ASSEMBLE_FLOPS = 40_000_000
FIRST_SCALE = 1.0 / (1.0 - BETA_ONE**STEP_COUNT)
SECOND_SCALE = 1.0 / (1.0 - BETA_TWO**STEP_COUNT)
MESH = pl.DeviceIdType.MESH


def grad_spec(col_split):
    return P("data", None, None, "model") if col_split else P("data", None, "model", None)


def state_spec(col_split):
    return P(None, "data", "model") if col_split else P(None, ("model", "data"), None)


def replica_spec(col_split):
    return P(None, None, "model") if col_split else P(None, "model", None)


def split(refs, *sizes):
    groups, start = [], 0
    for size in sizes:
        groups.append(refs[start] if size is None else refs[start : start + size])
        start += 1 if size is None else size
    return groups


def pack_rest(dst, proj, fcin, fcout):
    start = 0
    for rows in (fcin, fcout, proj):
        dst[start : start + rows.shape[0], :] = rows.astype(jnp.bfloat16)
        start += rows.shape[0]


def pack_grad(dst, qkv):
    for half in range(2):
        side = slice(half * LANES, half * LANES + LANES)
        first = half * 32
        dst[144:176, side] = qkv[first : first + 32, :LANES].astype(jnp.bfloat16)
        thin = qkv[first : first + 32, LANES:]
        dst[176:192, side] = jnp.concatenate([thin[:16], thin[16:]], axis=1).astype(jnp.bfloat16)


def pack_turned(dst, qkv):
    turned = jnp.transpose(qkv)
    blocks = [turned[THIRD * q : THIRD * (q + 1)] for q in range(4)]
    for half in range(2):
        side = slice(half * LANES, half * LANES + LANES)
        dst[144:192, side] = jnp.concatenate([blocks[half], blocks[half + 2]], axis=1).astype(jnp.bfloat16)


def column_sums(scr):
    folded = scr[:, :LANES] + scr[:, LANES:]
    return jnp.sum(jnp.transpose(folded), axis=0, keepdims=True)


def step_kernel(*refs):
    operands, out_g, (out_coef, out_ratio, out_far), out_b, buffers, singles, sems = split(
        refs, KINDS * 4, KINDS, 3, len(CHUNKS), KINDS * 5, 10, 9
    )
    grads, weights, firsts, seconds = split(operands, *[KINDS] * 4)
    stage, w_buf, m_buf, v_buf, g_buf = split(buffers, *[KINDS] * 5)
    turned, snd, rcv, n_acc, wn_acc, un_acc, coef, ratio, sync_src, sync_buf = singles
    load_sem, state_sem, send_sem, recv_sem, sync_send, sync_recv, far_sem, out_sem, grad_sem = sems

    d = lax.axis_index("data")
    m = lax.axis_index("model")

    def flipped(index, bits):
        high, low = (index // 2 + bits // 2) % 2, (index + bits) % 2
        return 2 * high + low

    peers = [(s, (flipped(m, s // DATA), flipped(d, s % DATA))) for s in range(DEVICES - 1, 0, -1)]

    def loads(layer, slot):
        return [pltpu.make_async_copy(grads[a].at[0, layer], stage[a].at[slot], load_sem.at[slot, a]) for a in range(KINDS)]

    for layer in range(SLOTS):
        for copy in loads(layer, layer):
            copy.start()

    barrier = pltpu.get_barrier_semaphore()

    for _, peer in peers:
        pl.semaphore_signal(barrier, inc=1, device_id=peer, device_id_type=MESH)

    def exchange(layer, k):
        return pltpu.make_async_remote_copy(
            src_ref=snd.at[k - 1, layer],
            dst_ref=rcv.at[k, layer],
            send_sem=send_sem.at[k - 1, layer],
            recv_sem=recv_sem.at[k - 1, layer],
            device_id=(m, (d + k) % DATA),
            device_id_type=MESH,
        )

    def produce(layer, opening=False):
        slot = lax.rem(layer, SLOTS)
        for copy in loads(layer, slot):
            copy.wait()
        turned[...] = jnp.transpose(stage[0][slot])
        for k in (2, 1, 3, 0):
            owner = (d + k) % DATA
            big = pl.ds(pl.multiple_of(owner * 64, 64), 64)
            small = pl.ds(pl.multiple_of(owner * 16, 16), 16)
            dst = snd.at[k - 1, layer] if k else rcv.at[0, layer]
            pack_rest(dst, stage[1][slot, small, :], stage[2][slot, big, :], stage[3][slot, big, :])
            pack_grad(dst, turned[big, :])
            if k and not opening:
                exchange(layer, k).start()
        if opening:
            pl.semaphore_wait(barrier, DEVICES - 1)
            for k in (2, 1, 3):
                exchange(layer, k).start()

        @pl.when(layer + SLOTS < LAYERS)
        def _():
            for copy in loads(layer + SLOTS, slot):
                copy.start()

    def produce_loop(layer, carry):
        produce(layer)
        return carry

    produce(jnp.int32(0), opening=True)
    lax.fori_loop(1, AHEAD, produce_loop, 0)

    state_copies = []
    for idx, (source, target) in enumerate(((weights, w_buf), (firsts, m_buf), (seconds, v_buf))):
        for a in range(KINDS):
            copy = pltpu.make_async_copy(source[a], target[a], state_sem.at[idx, a])
            copy.start()
            state_copies.append(copy)
    n_acc[...] = jnp.zeros_like(n_acc)
    wn_acc[...] = jnp.zeros_like(wn_acc)
    un_acc[...] = jnp.zeros_like(un_acc)
    for copy in state_copies:
        copy.wait()

    def grad_copy(a, group):
        part = pl.ds(group * GROUP, GROUP)
        return pltpu.make_async_copy(g_buf[a].at[part], out_g[a].at[part], grad_sem.at[a, group])

    def consume(layer, carry):
        @pl.when(layer + AHEAD < LAYERS)
        def _():
            produce(layer + AHEAD)

        for a in range(KINDS):
            w = w_buf[a][layer]
            wn_acc[pl.ds(a * LAYERS + layer, 1), 0 : COLS[a]] = jnp.sum(w * w, axis=0, keepdims=True)
            m_buf[a][layer] = (BETA_ONE * FIRST_SCALE) * m_buf[a][layer]
            v_buf[a][layer] = (BETA_TWO * SECOND_SCALE) * v_buf[a][layer]
        for k in (1, 2, 3):
            exchange(layer, k).wait_recv()

        def gathered(first, rows):
            parts = [rcv[k, layer, first : first + rows, :].astype(jnp.float32) for k in range(4)]
            return (parts[0] + parts[1] + parts[2] + parts[3]) * (1.0 / DATA)

        def squares(x):
            rows, cols = x.shape
            return jnp.sum((x * x).reshape(rows // 8, 8, cols), axis=0)

        fcin = gathered(0, 64)
        g_buf[2][layer] = fcin
        fcout = gathered(64, 64)
        g_buf[3][layer] = fcout
        proj = gathered(128, 16)
        g_buf[1][layer] = proj
        wide = gathered(144, 32)
        for half in range(2):
            g_buf[0][layer, 32 * half : 32 * half + 32, :LANES] = wide[:, LANES * half : LANES * half + LANES]
        thin = gathered(176, 16)
        for q in range(4):
            g_buf[0][layer, 16 * q : 16 * q + 16, LANES:] = thin[:, 64 * q : 64 * q + 64]
        n_acc[...] += squares(fcin) + squares(fcout) + squares(proj) + squares(wide) + squares(thin)

        @pl.when(lax.rem(layer, GROUP) == GROUP - 1)
        def _():
            for a in range(KINDS):
                grad_copy(a, layer // GROUP).start()

        return carry

    lax.fori_loop(0, LAYERS, consume, 0)

    def tile_copies(phase):
        return [
            pltpu.make_async_remote_copy(
                src_ref=sync_src.at[phase],
                dst_ref=sync_buf.at[phase, s],
                send_sem=sync_send.at[phase, s],
                recv_sem=sync_recv.at[phase, s],
                device_id=peer,
                device_id_type=MESH,
            )
            for s, peer in peers
        ]

    def share(phase, tile):
        sync_src[phase] = tile
        for copy in tile_copies(phase):
            copy.start()
        sync_buf[phase, 0] = tile

    def collect(phase):
        for copy in tile_copies(phase):
            copy.wait_recv()
        return jnp.sum(sync_buf[phase], axis=0)

    share(0, jnp.sum(n_acc[:, :LANES] + n_acc[:, LANES:], axis=0, keepdims=True))
    share(1, column_sums(wn_acc))
    total_norm = jnp.sqrt(jnp.sum(collect(0), axis=1, keepdims=True))
    clip_coef = jnp.minimum(1.0, MAX_NORM / total_norm)
    coef[...] = jnp.broadcast_to(clip_coef, coef.shape)
    first_coef = ((1.0 - BETA_ONE) * FIRST_SCALE) * clip_coef
    second_coef = ((1.0 - BETA_TWO) * SECOND_SCALE) * clip_coef * clip_coef

    def direction(layer, carry):
        for a in range(KINDS):
            g = g_buf[a][layer]
            first_hat = m_buf[a][layer] + first_coef * g
            second_hat = v_buf[a][layer] + second_coef * (g * g)
            u = first_hat / (jnp.sqrt(second_hat) + ADAM_EPS) + DECAY_RATE * w_buf[a][layer]
            m_buf[a][layer] = u
            un_acc[pl.ds(a * LAYERS + layer, 1), 0 : COLS[a]] = jnp.sum(u * u, axis=0, keepdims=True)
        return carry

    def set_ratio(weight_sq, update_sq):
        scaled = LEARN_RATE * (jnp.sqrt(weight_sq) / jnp.sqrt(update_sq))
        spread = jnp.transpose(jnp.broadcast_to(scaled, (LANES, LANES)))
        ratio[:, :LANES] = spread
        ratio[:, LANES:] = spread

    def finish(layer, carry):
        rows = []
        for a in range(KINDS):
            factor = ratio[pl.ds(a * LAYERS + layer, 1), 0 : COLS[a]]
            rows.append(w_buf[a][layer] - factor * m_buf[a][layer])
        pack_rest(snd.at[0, layer], *rows[1:])
        pack_turned(snd.at[0, layer], rows[0])
        return carry

    def sent(layer, carry):
        for k in (1, 2, 3):
            exchange(layer, k).wait_send()
        return carry

    starts = [sum(CHUNKS[:i]) for i in range(len(CHUNKS))]

    def replica_copy(i):
        return pltpu.make_async_copy(snd.at[0, pl.ds(starts[i], CHUNKS[i])], out_b[i], out_sem.at[i])

    def far(layer):
        return pltpu.make_async_remote_copy(
            src_ref=snd.at[0, layer],
            dst_ref=out_far.at[layer],
            send_sem=far_sem.at[0, layer],
            recv_sem=far_sem.at[1, layer],
            device_id=(m, (d + 2) % DATA),
            device_id_type=MESH,
        )

    def finish_and_send(layer, carry):
        finish(layer, carry)

        @pl.when(d % 2 == 1)
        def _():
            far(layer).start()

        return carry

    def send_late(layer, carry):
        @pl.when(d % 2 == 0)
        def _():
            far(layer).start()

        return carry

    def far_done(layer, carry):
        far(layer).wait()
        return carry

    coef_copy = pltpu.make_async_copy(coef, out_coef, out_sem.at[len(CHUNKS)])
    ratio_copy = pltpu.make_async_copy(ratio, out_ratio, out_sem.at[len(CHUNKS) + 1])

    lane = lax.broadcasted_iota(jnp.int32, (1, LANES), 1) % LAYERS
    lax.fori_loop(0, HEAD, direction, 0)
    share(2, column_sums(un_acc))
    coef_copy.start()
    lax.fori_loop(0, LAYERS, sent, 0)
    lax.fori_loop(HEAD, LAYERS, direction, 0)
    share(3, column_sums(un_acc))
    weight_sq = collect(1)
    set_ratio(weight_sq, jnp.where(lane < HEAD, collect(2), 1.0))
    lax.fori_loop(0, HEAD, finish_and_send, 0)
    replica_copy(0).start()
    set_ratio(weight_sq, collect(3))
    ratio_copy.start()
    lax.fori_loop(0, HEAD, send_late, 0)
    for i in range(1, len(CHUNKS)):
        lax.fori_loop(starts[i], starts[i] + CHUNKS[i], finish, 0)
        replica_copy(i).start()

    for phase in range(PHASES):
        for copy in tile_copies(phase):
            copy.wait_send()
    coef_copy.wait()
    ratio_copy.wait()
    for group in range(LAYERS // GROUP):
        for a in range(KINDS):
            grad_copy(a, group).wait()
    for i in range(len(CHUNKS)):
        replica_copy(i).wait()
    lax.fori_loop(0, HEAD, far_done, 0)


def run_step(grads, weights, firsts, seconds):
    state_shapes = [jax.ShapeDtypeStruct(w.shape, jnp.float32) for w in weights]
    pieces = [jax.ShapeDtypeStruct((n, PACKED, 256), jnp.bfloat16) for n in CHUNKS]
    row = (1, LANES)
    table = (LANES, WIDE)
    small = [jax.ShapeDtypeStruct(shape, jnp.float32) for shape in (row, table)]
    scratch = [pltpu.VMEM((SLOTS, *g.shape[2:]), jnp.float32) for g in grads]
    scratch += [pltpu.VMEM((LAYERS, ROWS[a], COLS[a]), jnp.float32) for a in range(KINDS)] * 4
    scratch += [pltpu.VMEM((WIDE, COLS[0]), jnp.float32)]
    scratch += [pltpu.VMEM((n, LAYERS, PACKED, WIDE), jnp.bfloat16) for n in (DATA - 1, DATA)]
    shapes = [(8, WIDE), table, table, row, table, (PHASES, *row), (PHASES, DEVICES, *row)]
    scratch += [pltpu.VMEM(shape, jnp.float32) for shape in shapes]
    exchange_shape = (DATA - 1, LAYERS)
    sync_shape = (PHASES, DEVICES)
    shapes = [(SLOTS, KINDS), (3, KINDS), exchange_shape, exchange_shape, sync_shape, sync_shape]
    shapes += [(2, HEAD), (len(CHUNKS) + 2,), (KINDS, LAYERS // GROUP)]
    scratch += [pltpu.SemaphoreType.DMA(shape) for shape in shapes]
    anywhere = pl.BlockSpec(memory_space=pl.ANY)
    out_shape = state_shapes + small + [pieces[0]] + pieces
    results = pl.pallas_call(
        step_kernel,
        out_shape=out_shape,
        in_specs=[anywhere] * (KINDS * 4),
        out_specs=[anywhere] * len(out_shape),
        scratch_shapes=scratch,
        compiler_params=pltpu.CompilerParams(collective_id=0, has_side_effects=True, vmem_limit_bytes=63 << 20),
        name="lamb_step",
    )(*grads, *weights, *firsts, *seconds)
    return split(results, KINDS, None, None, None, len(CHUNKS))


def update_kernel(*refs):
    coef, ratio, means, weights, firsts, seconds, out_w, out_m, out_v = split(refs, None, None, *[KINDS] * 7)
    clip_coef = coef[:, :1]
    block = means[0].shape[0]
    for b in range(block):
        layer = pl.program_id(0) * block + b
        for a in range(KINDS):
            w = weights[a][b]
            clipped = clip_coef * means[a][b]
            first = BETA_ONE * firsts[a][b] + (1.0 - BETA_ONE) * clipped
            second = BETA_TWO * seconds[a][b] + (1.0 - BETA_TWO) * clipped * clipped
            out_m[a][b] = first
            out_v[a][b] = second
            u = (first * FIRST_SCALE) / (jnp.sqrt(second * SECOND_SCALE) + ADAM_EPS) + DECAY_RATE * w
            out_w[a][b] = w - ratio[pl.ds(a * LAYERS + layer, 1), 0 : COLS[a]] * u


def update(coef, ratio, means, weights, firsts, seconds):
    block = 2
    layer_specs = [pl.BlockSpec((block, ROWS[a], COLS[a]), lambda i: (i, 0, 0)) for a in range(KINDS)]
    return pl.pallas_call(
        update_kernel,
        grid=(LAYERS // block,),
        out_shape=[jax.ShapeDtypeStruct(w.shape, jnp.float32) for w in weights] * 3,
        in_specs=[pl.BlockSpec(table.shape, lambda i: (0, 0)) for table in (coef, ratio)] + layer_specs * 4,
        out_specs=layer_specs * 3,
        cost_estimate=pl.CostEstimate(flops=UPDATE_FLOPS, bytes_accessed=47_000_000, transcendentals=0),
        compiler_params=pltpu.CompilerParams(vmem_limit_bytes=60 << 20),
        name="update",
    )(coef, ratio, *means, *weights, *firsts, *seconds)


def assemble_kernel(has_alias, *refs):
    shards, _, (qkv, proj, fcin, fcout), parts = split(refs, DATA, KINDS * has_alias, KINDS, None)
    d = lax.axis_index("data")
    partner = d + 1 - 2 * (d % 2)
    owners = (d, (d + 2) % DATA, partner, (partner + 2) % DATA)
    for owner, shard in zip(owners, shards):
        big = pl.ds(pl.multiple_of(owner * 64, 64), 64)
        small = pl.ds(pl.multiple_of(owner * 16, 16), 16)
        fcin[:, big, :] = shard[:, 0:64, :]
        fcout[:, big, :] = shard[:, 64:128, :]
        proj[:, small, :] = shard[:, 128:144, :]
        parts[owner] = shard[:, 144:192, :]
    for half in range(2):
        side = slice(half * LANES, half * LANES + LANES)
        first, second = parts[2 * half], parts[2 * half + 1]
        for q in range(4):
            lane = (q % 2) * LANES + (q // 2) * 64
            pair = jnp.concatenate([shard[:, :, lane : lane + 64] for shard in (first, second)], axis=2)
            qkv[:, THIRD * q : THIRD * (q + 1), side] = pair


def assemble(chunk, shards, previous):
    block = 2
    shapes = [(LAYERS, 192, 256), (LAYERS, 64, 256), (LAYERS, 256, 256), (LAYERS, 256, 256)]
    first = sum(CHUNKS[:chunk]) // block
    in_specs = [pl.BlockSpec((block, PACKED, 256), lambda i: (i, 0, 0))] * 4
    in_specs += [pl.BlockSpec(memory_space=pl.ANY)] * len(previous)
    return pl.pallas_call(
        functools.partial(assemble_kernel, bool(previous)),
        grid=(CHUNKS[chunk] // block,),
        out_shape=[jax.ShapeDtypeStruct(s, jnp.bfloat16) for s in shapes],
        in_specs=in_specs,
        out_specs=[pl.BlockSpec((block, s[1], s[2]), lambda i: (first + i, 0, 0)) for s in shapes],
        scratch_shapes=[pltpu.VMEM((4, block, 48, 256), jnp.bfloat16)],
        input_output_aliases={4 + i: i for i in range(len(previous))},
        cost_estimate=pl.CostEstimate(flops=ASSEMBLE_FLOPS * CHUNKS[chunk], bytes_accessed=800_000 * CHUNKS[chunk], transcendentals=0),
        compiler_params=pltpu.CompilerParams(vmem_limit_bytes=24 << 20),
        name="assemble",
    )(*shards, *previous)


def solution(mesh):
    in_specs = []
    for col_split in COLUMN_SPLIT:
        in_specs.extend([grad_spec(col_split), state_spec(col_split), state_spec(col_split), state_spec(col_split)])
    out_specs = tuple([replica_spec(col_split) for col_split in COLUMN_SPLIT] + [state_spec(col_split) for col_split in COLUMN_SPLIT] * 3)

    across = [(i, (i + 2) % DATA) for i in range(DATA)]
    on_chip = [(i, i + 1 - 2 * (i % 2)) for i in range(DATA)]

    def device_step(*arrays):
        grads, weights, firsts, seconds = (arrays[i::4] for i in range(4))
        grads = (jnp.swapaxes(grads[0], 2, 3), *grads[1:])
        means, coef, ratio, far_head, pieces = run_step(grads, weights, firsts, seconds)
        states = update(coef, ratio, means, weights, firsts, seconds)
        replicas = ()
        for chunk, own in enumerate(pieces):
            far = lax.ppermute(own, "data", across) if chunk else far_head
            near = lax.ppermute(own, "data", on_chip)
            far_near = lax.ppermute(far, "data", on_chip)
            replicas = assemble(chunk, (own, far, near, far_near), tuple(replicas))
        return (jnp.swapaxes(replicas[0], 1, 2), *replicas[1:], *states)

    return jax.shard_map(device_step, mesh=mesh, in_specs=tuple(in_specs), out_specs=out_specs, check_vma=False)
```

```python
import functools

import jax
import jax.numpy as jnp
from jax import lax
from jax.experimental import pallas as pl
from jax.experimental.pallas import tpu as pltpu
from jax.sharding import PartitionSpec as P


LEARN_RATE = 0.08
BETA_ONE = 0.9
BETA_TWO = 0.999
ADAM_EPS = 1e-6
DECAY_RATE = 0.01
MAX_NORM = 1.0
STEP_COUNT = 100
COLUMN_SPLIT = (True, False, True, False)

LAYERS = 32
DATA = 4
DEVICES = 16
ROWS = (64, 16, 64, 64)
COLS = (192, 256, 256, 256)
KINDS = 4
LANES = 128
WIDE = 256
THIRD = 48
PACKED = 192
PHASES = 4
SLOTS = 3
AHEAD = 6
GROUP = 8
CHUNKS = (8, 8, 8, 4, 2, 2)
HEAD = CHUNKS[0]
EARLY = 6
FIRST = 3
MIDDLE = 26
UPDATE_FLOPS = 2_000_000_000
ASSEMBLE_FLOPS = 40_000_000
FIRST_SCALE = 1.0 / (1.0 - BETA_ONE**STEP_COUNT)
SECOND_SCALE = 1.0 / (1.0 - BETA_TWO**STEP_COUNT)
MESH = pl.DeviceIdType.MESH


def grad_spec(col_split):
    return P("data", None, None, "model") if col_split else P("data", None, "model", None)


def state_spec(col_split):
    return P(None, "data", "model") if col_split else P(None, ("model", "data"), None)


def replica_spec(col_split):
    return P(None, None, "model") if col_split else P(None, "model", None)


def split(refs, *sizes):
    groups, start = [], 0
    for size in sizes:
        groups.append(refs[start] if size is None else refs[start : start + size])
        start += 1 if size is None else size
    return groups


def pack_rest(dst, proj, fcin, fcout):
    start = 0
    for rows in (fcin, fcout, proj):
        dst[start : start + rows.shape[0], :] = rows.astype(jnp.bfloat16)
        start += rows.shape[0]


def pack_grad(dst, qkv):
    for half in range(2):
        side = slice(half * LANES, half * LANES + LANES)
        first = half * 32
        dst[144:176, side] = qkv[first : first + 32, :LANES].astype(jnp.bfloat16)
        thin = qkv[first : first + 32, LANES:]
        dst[176:192, side] = jnp.concatenate([thin[:16], thin[16:]], axis=1).astype(jnp.bfloat16)


def pack_turned(dst, qkv):
    turned = jnp.transpose(qkv)
    blocks = [turned[THIRD * q : THIRD * (q + 1)] for q in range(4)]
    for half in range(2):
        side = slice(half * LANES, half * LANES + LANES)
        dst[144:192, side] = jnp.concatenate([blocks[half], blocks[half + 2]], axis=1).astype(jnp.bfloat16)


def column_sums(scr):
    folded = scr[:, :LANES] + scr[:, LANES:]
    return jnp.sum(jnp.transpose(folded), axis=0, keepdims=True)


def step_kernel(*refs):
    operands, out_g, (out_coef, out_ratio, out_far), out_b, buffers, singles, sems = split(
        refs, KINDS * 4, KINDS, 3, len(CHUNKS), KINDS * 5, 10, 9
    )
    grads, weights, firsts, seconds = split(operands, *[KINDS] * 4)
    stage, w_buf, m_buf, v_buf, g_buf = split(buffers, *[KINDS] * 5)
    turned, snd, rcv, n_acc, wn_acc, un_acc, coef, ratio, sync_src, sync_buf = singles
    load_sem, state_sem, send_sem, recv_sem, sync_send, sync_recv, far_sem, out_sem, grad_sem = sems

    d = lax.axis_index("data")
    m = lax.axis_index("model")

    def flipped(index, bits):
        high, low = (index // 2 + bits // 2) % 2, (index + bits) % 2
        return 2 * high + low

    peers = [(s, (flipped(m, s // DATA), flipped(d, s % DATA))) for s in range(DEVICES - 1, 0, -1)]

    def loads(layer, slot):
        return [pltpu.make_async_copy(grads[a].at[0, layer], stage[a].at[slot], load_sem.at[slot, a]) for a in range(KINDS)]

    for layer in range(SLOTS):
        for copy in loads(layer, layer):
            copy.start()

    barrier = pltpu.get_barrier_semaphore()

    for _, peer in peers:
        pl.semaphore_signal(barrier, inc=1, device_id=peer, device_id_type=MESH)

    def exchange(layer, k):
        return pltpu.make_async_remote_copy(
            src_ref=snd.at[k - 1, layer],
            dst_ref=rcv.at[k, layer],
            send_sem=send_sem.at[k - 1, layer],
            recv_sem=recv_sem.at[k - 1, layer],
            device_id=(m, (d + k) % DATA),
            device_id_type=MESH,
        )

    def produce(layer, opening=False):
        slot = lax.rem(layer, SLOTS)
        for copy in loads(layer, slot):
            copy.wait()
        turned[...] = jnp.transpose(stage[0][slot])
        for k in (2, 1, 3, 0):
            owner = (d + k) % DATA
            big = pl.ds(pl.multiple_of(owner * 64, 64), 64)
            small = pl.ds(pl.multiple_of(owner * 16, 16), 16)
            dst = snd.at[k - 1, layer] if k else rcv.at[0, layer]
            pack_rest(dst, stage[1][slot, small, :], stage[2][slot, big, :], stage[3][slot, big, :])
            pack_grad(dst, turned[big, :])
            if k and not opening:
                exchange(layer, k).start()
        if opening:
            pl.semaphore_wait(barrier, DEVICES - 1)
            for k in (2, 1, 3):
                exchange(layer, k).start()

        @pl.when(layer + SLOTS < LAYERS)
        def _():
            for copy in loads(layer + SLOTS, slot):
                copy.start()

    def produce_loop(layer, carry):
        produce(layer)
        return carry

    produce(jnp.int32(0), opening=True)
    lax.fori_loop(1, AHEAD, produce_loop, 0)

    state_copies = []
    for idx, (source, target) in enumerate(((weights, w_buf), (firsts, m_buf), (seconds, v_buf))):
        for a in range(KINDS):
            copy = pltpu.make_async_copy(source[a], target[a], state_sem.at[idx, a])
            copy.start()
            state_copies.append(copy)
    n_acc[...] = jnp.zeros_like(n_acc)
    wn_acc[...] = jnp.zeros_like(wn_acc)
    un_acc[...] = jnp.zeros_like(un_acc)
    for copy in state_copies:
        copy.wait()

    def grad_copy(a, group):
        part = pl.ds(group * GROUP, GROUP)
        return pltpu.make_async_copy(g_buf[a].at[part], out_g[a].at[part], grad_sem.at[a, group])

    def consume(layer, carry):
        @pl.when(layer + AHEAD < LAYERS)
        def _():
            produce(layer + AHEAD)

        for a in range(KINDS):
            w = w_buf[a][layer]
            wn_acc[pl.ds(a * LAYERS + layer, 1), 0 : COLS[a]] = jnp.sum(w * w, axis=0, keepdims=True)
            m_buf[a][layer] = (BETA_ONE * FIRST_SCALE) * m_buf[a][layer]
            v_buf[a][layer] = (BETA_TWO * SECOND_SCALE) * v_buf[a][layer]
        for k in (1, 2, 3):
            exchange(layer, k).wait_recv()

        def gathered(first, rows):
            parts = [rcv[k, layer, first : first + rows, :].astype(jnp.float32) for k in range(4)]
            return (parts[0] + parts[1] + parts[2] + parts[3]) * (1.0 / DATA)

        def squares(x):
            rows, cols = x.shape
            return jnp.sum((x * x).reshape(rows // 8, 8, cols), axis=0)

        fcin = gathered(0, 64)
        g_buf[2][layer] = fcin
        fcout = gathered(64, 64)
        g_buf[3][layer] = fcout
        proj = gathered(128, 16)
        g_buf[1][layer] = proj
        wide = gathered(144, 32)
        for half in range(2):
            g_buf[0][layer, 32 * half : 32 * half + 32, :LANES] = wide[:, LANES * half : LANES * half + LANES]
        thin = gathered(176, 16)
        for q in range(4):
            g_buf[0][layer, 16 * q : 16 * q + 16, LANES:] = thin[:, 64 * q : 64 * q + 64]
        n_acc[...] += squares(fcin) + squares(fcout) + squares(proj) + squares(wide) + squares(thin)

        @pl.when(lax.rem(layer, GROUP) == GROUP - 1)
        def _():
            for a in range(KINDS):
                grad_copy(a, layer // GROUP).start()

        return carry

    lax.fori_loop(0, LAYERS, consume, 0)

    def tile_copies(phase):
        return [
            pltpu.make_async_remote_copy(
                src_ref=sync_src.at[phase],
                dst_ref=sync_buf.at[phase, s],
                send_sem=sync_send.at[phase, s],
                recv_sem=sync_recv.at[phase, s],
                device_id=peer,
                device_id_type=MESH,
            )
            for s, peer in peers
        ]

    def share(phase, tile):
        sync_src[phase] = tile
        for copy in tile_copies(phase):
            copy.start()
        sync_buf[phase, 0] = tile

    def collect(phase):
        for copy in tile_copies(phase):
            copy.wait_recv()
        return jnp.sum(sync_buf[phase], axis=0)

    share(0, jnp.sum(n_acc[:, :LANES] + n_acc[:, LANES:], axis=0, keepdims=True))
    share(1, column_sums(wn_acc))
    total_norm = jnp.sqrt(jnp.sum(collect(0), axis=1, keepdims=True))
    clip_coef = jnp.minimum(1.0, MAX_NORM / total_norm)
    coef[...] = jnp.broadcast_to(clip_coef, coef.shape)
    first_coef = ((1.0 - BETA_ONE) * FIRST_SCALE) * clip_coef
    second_coef = ((1.0 - BETA_TWO) * SECOND_SCALE) * clip_coef * clip_coef

    def direction(layer, carry):
        for a in range(KINDS):
            g = g_buf[a][layer]
            first_hat = m_buf[a][layer] + first_coef * g
            second_hat = v_buf[a][layer] + second_coef * (g * g)
            u = first_hat / (jnp.sqrt(second_hat) + ADAM_EPS) + DECAY_RATE * w_buf[a][layer]
            m_buf[a][layer] = u
            un_acc[pl.ds(a * LAYERS + layer, 1), 0 : COLS[a]] = jnp.sum(u * u, axis=0, keepdims=True)
        return carry

    def set_ratio(weight_sq, update_sq):
        scaled = LEARN_RATE * (jnp.sqrt(weight_sq) / jnp.sqrt(update_sq))
        spread = jnp.transpose(jnp.broadcast_to(scaled, (LANES, LANES)))
        ratio[:, :LANES] = spread
        ratio[:, LANES:] = spread

    def finish(layer, carry):
        rows = []
        for a in range(KINDS):
            factor = ratio[pl.ds(a * LAYERS + layer, 1), 0 : COLS[a]]
            rows.append(w_buf[a][layer] - factor * m_buf[a][layer])
        pack_rest(snd.at[0, layer], *rows[1:])
        pack_turned(snd.at[0, layer], rows[0])
        return carry

    def sent(*steps):
        def wait_sent(layer, carry):
            for k in steps:
                exchange(layer, k).wait_send()
            return carry

        lax.fori_loop(0, LAYERS, wait_sent, 0)

    starts = [sum(CHUNKS[:i]) for i in range(len(CHUNKS))]

    def replica_copy(i):
        return pltpu.make_async_copy(snd.at[0, pl.ds(starts[i], CHUNKS[i])], out_b[i], out_sem.at[i])

    def far(layer):
        return pltpu.make_async_remote_copy(
            src_ref=snd.at[0, layer],
            dst_ref=out_far.at[layer],
            send_sem=far_sem.at[0, layer],
            recv_sem=far_sem.at[1, layer],
            device_id=(m, (d + 2) % DATA),
            device_id_type=MESH,
        )

    def finish_and_send(layer, carry):
        finish(layer, carry)

        @pl.when(d % 2 == 1)
        def _():
            far(layer).start()

        return carry

    def send_late(layer, carry):
        @pl.when(d % 2 == 0)
        def _():
            far(layer).start()

        return carry

    def far_done(layer, carry):
        far(layer).wait()
        return carry

    coef_copy = pltpu.make_async_copy(coef, out_coef, out_sem.at[len(CHUNKS)])
    ratio_copy = pltpu.make_async_copy(ratio, out_ratio, out_sem.at[len(CHUNKS) + 1])

    lane = lax.broadcasted_iota(jnp.int32, (1, LANES), 1) % LAYERS
    lax.fori_loop(0, EARLY, direction, 0)
    share(2, column_sums(un_acc))
    sent(1)
    lax.fori_loop(EARLY, MIDDLE, direction, 0)
    weight_sq = collect(1)
    set_ratio(weight_sq, jnp.where(lane < EARLY, collect(2), 1.0))
    lax.fori_loop(0, FIRST, finish_and_send, 0)
    lax.fori_loop(MIDDLE, LAYERS, direction, 0)
    share(3, column_sums(un_acc))
    lax.fori_loop(FIRST, EARLY, finish_and_send, 0)
    coef_copy.start()
    sent(2, 3)
    set_ratio(weight_sq, collect(3))
    ratio_copy.start()
    lax.fori_loop(EARLY, HEAD, finish_and_send, 0)
    replica_copy(0).start()
    lax.fori_loop(0, HEAD, send_late, 0)
    for i in range(1, len(CHUNKS)):
        lax.fori_loop(starts[i], starts[i] + CHUNKS[i], finish, 0)
        replica_copy(i).start()

    for phase in range(PHASES):
        for copy in tile_copies(phase):
            copy.wait_send()
    coef_copy.wait()
    ratio_copy.wait()
    for group in range(LAYERS // GROUP):
        for a in range(KINDS):
            grad_copy(a, group).wait()
    for i in range(len(CHUNKS)):
        replica_copy(i).wait()
    lax.fori_loop(0, HEAD, far_done, 0)


def run_step(grads, weights, firsts, seconds):
    state_shapes = [jax.ShapeDtypeStruct(w.shape, jnp.float32) for w in weights]
    pieces = [jax.ShapeDtypeStruct((n, PACKED, 256), jnp.bfloat16) for n in CHUNKS]
    row = (1, LANES)
    table = (LANES, WIDE)
    small = [jax.ShapeDtypeStruct(shape, jnp.float32) for shape in (row, table)]
    scratch = [pltpu.VMEM((SLOTS, *g.shape[2:]), jnp.float32) for g in grads]
    scratch += [pltpu.VMEM((LAYERS, ROWS[a], COLS[a]), jnp.float32) for a in range(KINDS)] * 4
    scratch += [pltpu.VMEM((WIDE, COLS[0]), jnp.float32)]
    scratch += [pltpu.VMEM((n, LAYERS, PACKED, WIDE), jnp.bfloat16) for n in (DATA - 1, DATA)]
    shapes = [(8, WIDE), table, table, row, table, (PHASES, *row), (PHASES, DEVICES, *row)]
    scratch += [pltpu.VMEM(shape, jnp.float32) for shape in shapes]
    exchange_shape = (DATA - 1, LAYERS)
    sync_shape = (PHASES, DEVICES)
    shapes = [(SLOTS, KINDS), (3, KINDS), exchange_shape, exchange_shape, sync_shape, sync_shape]
    shapes += [(2, HEAD), (len(CHUNKS) + 2,), (KINDS, LAYERS // GROUP)]
    scratch += [pltpu.SemaphoreType.DMA(shape) for shape in shapes]
    anywhere = pl.BlockSpec(memory_space=pl.ANY)
    out_shape = state_shapes + small + [pieces[0]] + pieces
    results = pl.pallas_call(
        step_kernel,
        out_shape=out_shape,
        in_specs=[anywhere] * (KINDS * 4),
        out_specs=[anywhere] * len(out_shape),
        scratch_shapes=scratch,
        compiler_params=pltpu.CompilerParams(collective_id=0, has_side_effects=True, vmem_limit_bytes=63 << 20),
        name="lamb_step",
    )(*grads, *weights, *firsts, *seconds)
    return split(results, KINDS, None, None, None, len(CHUNKS))


def update_kernel(*refs):
    coef, ratio, means, weights, firsts, seconds, out_w, out_m, out_v = split(refs, None, None, *[KINDS] * 7)
    clip_coef = coef[:, :1]
    block = means[0].shape[0]
    for b in range(block):
        layer = pl.program_id(0) * block + b
        for a in range(KINDS):
            w = weights[a][b]
            clipped = clip_coef * means[a][b]
            first = BETA_ONE * firsts[a][b] + (1.0 - BETA_ONE) * clipped
            second = BETA_TWO * seconds[a][b] + (1.0 - BETA_TWO) * clipped * clipped
            out_m[a][b] = first
            out_v[a][b] = second
            u = (first * FIRST_SCALE) / (jnp.sqrt(second * SECOND_SCALE) + ADAM_EPS) + DECAY_RATE * w
            out_w[a][b] = w - ratio[pl.ds(a * LAYERS + layer, 1), 0 : COLS[a]] * u


def update(coef, ratio, means, weights, firsts, seconds):
    block = 2
    layer_specs = [pl.BlockSpec((block, ROWS[a], COLS[a]), lambda i: (i, 0, 0)) for a in range(KINDS)]
    return pl.pallas_call(
        update_kernel,
        grid=(LAYERS // block,),
        out_shape=[jax.ShapeDtypeStruct(w.shape, jnp.float32) for w in weights] * 3,
        in_specs=[pl.BlockSpec(table.shape, lambda i: (0, 0)) for table in (coef, ratio)] + layer_specs * 4,
        out_specs=layer_specs * 3,
        cost_estimate=pl.CostEstimate(flops=UPDATE_FLOPS, bytes_accessed=47_000_000, transcendentals=0),
        compiler_params=pltpu.CompilerParams(vmem_limit_bytes=60 << 20),
        name="update",
    )(coef, ratio, *means, *weights, *firsts, *seconds)


def assemble_kernel(has_alias, *refs):
    shards, _, (qkv, proj, fcin, fcout), parts = split(refs, DATA, KINDS * has_alias, KINDS, None)
    d = lax.axis_index("data")
    partner = d + 1 - 2 * (d % 2)
    owners = (d, (d + 2) % DATA, partner, (partner + 2) % DATA)
    for owner, shard in zip(owners, shards):
        big = pl.ds(pl.multiple_of(owner * 64, 64), 64)
        small = pl.ds(pl.multiple_of(owner * 16, 16), 16)
        fcin[:, big, :] = shard[:, 0:64, :]
        fcout[:, big, :] = shard[:, 64:128, :]
        proj[:, small, :] = shard[:, 128:144, :]
        parts[owner] = shard[:, 144:192, :]
    for half in range(2):
        side = slice(half * LANES, half * LANES + LANES)
        first, second = parts[2 * half], parts[2 * half + 1]
        for q in range(4):
            lane = (q % 2) * LANES + (q // 2) * 64
            pair = jnp.concatenate([shard[:, :, lane : lane + 64] for shard in (first, second)], axis=2)
            qkv[:, THIRD * q : THIRD * (q + 1), side] = pair


def assemble(chunk, shards, previous):
    block = 2
    shapes = [(LAYERS, 192, 256), (LAYERS, 64, 256), (LAYERS, 256, 256), (LAYERS, 256, 256)]
    first = sum(CHUNKS[:chunk]) // block
    in_specs = [pl.BlockSpec((block, PACKED, 256), lambda i: (i, 0, 0))] * 4
    in_specs += [pl.BlockSpec(memory_space=pl.ANY)] * len(previous)
    return pl.pallas_call(
        functools.partial(assemble_kernel, bool(previous)),
        grid=(CHUNKS[chunk] // block,),
        out_shape=[jax.ShapeDtypeStruct(s, jnp.bfloat16) for s in shapes],
        in_specs=in_specs,
        out_specs=[pl.BlockSpec((block, s[1], s[2]), lambda i: (first + i, 0, 0)) for s in shapes],
        scratch_shapes=[pltpu.VMEM((4, block, 48, 256), jnp.bfloat16)],
        input_output_aliases={4 + i: i for i in range(len(previous))},
        cost_estimate=pl.CostEstimate(flops=ASSEMBLE_FLOPS * CHUNKS[chunk], bytes_accessed=800_000 * CHUNKS[chunk], transcendentals=0),
        compiler_params=pltpu.CompilerParams(vmem_limit_bytes=24 << 20),
        name="assemble",
    )(*shards, *previous)


def solution(mesh):
    in_specs = []
    for col_split in COLUMN_SPLIT:
        in_specs.extend([grad_spec(col_split), state_spec(col_split), state_spec(col_split), state_spec(col_split)])
    out_specs = tuple([replica_spec(col_split) for col_split in COLUMN_SPLIT] + [state_spec(col_split) for col_split in COLUMN_SPLIT] * 3)

    across = [(i, (i + 2) % DATA) for i in range(DATA)]
    on_chip = [(i, i + 1 - 2 * (i % 2)) for i in range(DATA)]

    def device_step(*arrays):
        grads, weights, firsts, seconds = (arrays[i::4] for i in range(4))
        grads = (jnp.swapaxes(grads[0], 2, 3), *grads[1:])
        means, coef, ratio, far_head, pieces = run_step(grads, weights, firsts, seconds)
        states = update(coef, ratio, means, weights, firsts, seconds)
        replicas = ()
        for chunk, own in enumerate(pieces):
            far = lax.ppermute(own, "data", across) if chunk else far_head
            near = lax.ppermute(own, "data", on_chip)
            far_near = lax.ppermute(far, "data", on_chip)
            replicas = assemble(chunk, (own, far, near, far_near), tuple(replicas))
        return (jnp.swapaxes(replicas[0], 1, 2), *replicas[1:], *states)

    return jax.shard_map(device_step, mesh=mesh, in_specs=tuple(in_specs), out_specs=out_specs, check_vma=False)
```
